128 devices in a mesh: dp: 32 (over z, y, core), mp: 4 (over x).
Axes of the slice: x: 4, y: 4, z: 4, core: 2. Of those that a mesh axis runs over, the one named last changes fastest.
Arguments:
- queries: bfloat16 [1024, 64, 128], P('dp', 'mp'), may hold values from -8 to 8
- lookup_sheets: bfloat16 [32768, 16, 8, 128], P('dp', None, 'mp'), may hold values from -6 to 6
- content_sheets: bfloat16 [32768, 16, 8, 128], P('dp', None, 'mp'), may hold values from -12 to 12
- page_table: int32 [1024, 32], replicated, may hold values from 0 to 32767, as said below
- context_len: int32 [1024], replicated, may hold values from 32 to 512, as said below
- out_weight: bfloat16 [8192, 8192], P('mp', 'dp'), may hold values from -0.0625 to 0.0625
Outputs:
- attention: bfloat16 [1024, 64, 128], P('dp', 'mp')
- projected: bfloat16 [1024, 8192], P('mp', 'dp')
The draws below stay inside these ranges and needn't reach their ends.
Inputs may be any that keep to these rules, and one draw needn't show every extreme that they name: `page_table`: every entry names a pool page, 0 to 32767, and every pool page appears exactly once in the whole table. `context_len`: each length lies between 32 and 512; most contexts are short, and some request has exactly 512 tokens.
All inputs are finite; a program needn't handle non-finite values.
Results may differ from the reference program's by a relative error of at most 0.0015.
Values may be sent and summed in bfloat16 or wider, within the bound.
A program may use at most 128 MiB of HBM per device.

```python
import jax
import jax.numpy as jnp
from jax import lax

D = 8192
ASKER_COUNT = 64
LOOKUP_COUNT = 8
SPAN_PER_ASKER = 128
SHEET_CAPACITY = 16
REQ = 1024
SHEET_TOTAL = 32768
MAXPG = 32


def draw_context_len(key, part):
    key_len, key_pos = jax.random.split(jax.random.fold_in(key, 11))
    longest = MAXPG * SHEET_CAPACITY
    lowest = max(longest // 16, 1)
    drawn = jax.random.randint(key_len, (REQ,), 0, longest, dtype=jnp.int32)
    skewed = drawn * drawn // longest * drawn // longest
    lengths = lowest + skewed * (longest - lowest) // longest
    chosen = jax.random.randint(key_pos, (), 0, REQ, dtype=jnp.int32)
    return lengths.at[chosen].set(longest).astype(jnp.int32)


def draw_page_table(key, part):
    shuffled = jax.random.permutation(jax.random.fold_in(key, 23), REQ * MAXPG)
    return shuffled.reshape(REQ, MAXPG).astype(jnp.int32)


def levels(key, dims, cuts, least, top_value):
    def one(axis_at, shards_of):
        steps = jax.random.uniform(jax.random.fold_in(jax.random.fold_in(key, 6), axis_at), (shards_of,), jnp.float32, least / len(cuts), top_value / len(cuts))
        return jnp.repeat(jnp.exp(steps), dims[axis_at] // shards_of).reshape((-1,) + (1,) * (len(dims) - axis_at - 1))

    gain = one(*cuts[0])
    for cut in cuts[1:]:
        gain = gain * one(*cut)
    return gain


def bell_draw(rng, extent, width, reach, pieces=(), kind=jnp.bfloat16):
    loudness = levels(rng, extent, pieces, -0.22, 0.18) if pieces else 1.0
    values = jax.random.normal(rng, extent, jnp.float32) * width * loudness
    return jnp.minimum(jnp.maximum(values, -reach), reach).astype(kind)


def setup_inputs(seed: int = 0) -> dict:
    key_list = jax.random.split(jax.random.key(seed), 7)
    return {
        "queries": bell_draw(key_list[0], (REQ, ASKER_COUNT, SPAN_PER_ASKER), 1.5, 8.0, ((0, 32), (1, 4))),
        "lookup_sheets": bell_draw(key_list[1], (SHEET_TOTAL, SHEET_CAPACITY, LOOKUP_COUNT, SPAN_PER_ASKER), 1.0, 6.0, ((0, 32), (2, 4))),
        "content_sheets": bell_draw(key_list[2], (SHEET_TOTAL, SHEET_CAPACITY, LOOKUP_COUNT, SPAN_PER_ASKER), 2.0, 12.0, ((0, 32), (2, 4))),
        "page_table": draw_page_table(jax.random.fold_in(key_list[6], 71), 0),
        "context_len": draw_context_len(jax.random.fold_in(key_list[6], 71), 0),
        "out_weight": bell_draw(key_list[5], (ASKER_COUNT * SPAN_PER_ASKER, D), (ASKER_COUNT * SPAN_PER_ASKER) ** -0.5, 0.0625, ((0, 4), (1, 32))),
    }


def reference(queries, lookup_sheets, content_sheets, page_table, context_len, out_weight):
    cluster_member = ASKER_COUNT // LOOKUP_COUNT

    def one_request(inputs):
        asker_vector, page_ids, length = inputs
        keys = lookup_sheets[page_ids].astype(jnp.float32)
        values = content_sheets[page_ids].astype(jnp.float32)
        clustered_askers = asker_vector.reshape(LOOKUP_COUNT, cluster_member, SPAN_PER_ASKER).astype(jnp.float32)
        scores = jnp.einsum("kgd,ptkd->kgpt", clustered_askers, keys) * (SPAN_PER_ASKER ** -0.5)
        position = (jnp.arange(MAXPG, dtype=jnp.int32)[:, None] * SHEET_CAPACITY
                    + jnp.arange(SHEET_CAPACITY, dtype=jnp.int32)[None, :])
        is_valid = position < length
        scores = jnp.where(is_valid, scores, -1e30)
        page_peak = jnp.max(scores, axis=-1)
        weights = jnp.where(is_valid, jnp.exp(scores - page_peak[..., None]), 0.0)
        page_mass = jnp.sum(weights, axis=-1)
        rounded = lax.optimization_barrier(weights.astype(jnp.bfloat16)).astype(jnp.float32)
        page_acc = jnp.einsum("kgpt,ptkd->kgpd", rounded, values)
        peak_row = jnp.max(page_peak, axis=-1)
        factor = jnp.exp(page_peak - peak_row[..., None])
        acc_row = jnp.sum(page_acc * factor[..., None], axis=2)
        mass_row = jnp.sum(page_mass * factor, axis=2)
        return (acc_row / mass_row[..., None]).astype(jnp.bfloat16).reshape(ASKER_COUNT, SPAN_PER_ASKER)

    attention = lax.map(one_request, (queries, page_table, context_len))
    flat_rows = attention.reshape(attention.shape[0], ASKER_COUNT * SPAN_PER_ASKER)
    projected = jnp.dot(flat_rows, out_weight, preferred_element_type=jnp.float32).astype(jnp.bfloat16)
    return attention, projected
```

```python
import functools

import jax
import jax.numpy as jnp
from jax import lax
from jax.experimental import pallas as pl
from jax.experimental.pallas import tpu as pltpu
from jax.sharding import PartitionSpec as P

MESH = pl.DeviceIdType.MESH
NEG = -1e30
DEPTH = 4
PRE = 2
RING = 4


def axis_barrier(axes):
    barrier = pltpu.get_barrier_semaphore()
    total = 0
    for name in axes:
        n = lax.axis_size(name)
        me = lax.axis_index(name)
        for step in range(1, n):
            pl.semaphore_signal(
                barrier, inc=1, device_id={name: lax.rem(me + step, n)}, device_id_type=MESH
            )
        total += n - 1
    pl.semaphore_wait(barrier, total)


def place():
    me = lax.axis_index("dp")
    return lax.rem(me, 2), lax.rem(me // 2, RING), me // (2 * RING)


def spot(side, y, z):
    return (lax.rem(z + RING, RING) * RING + lax.rem(y + RING, RING)) * 2 + side


def torus_gather(buf, send_sem, recv_sem):
    side, y, z = place()
    me = spot(side, y, z)
    sent = []

    def piece(q, i, j, of=None):
        of = side if of is None else of
        return spot(of, y + i, z + j) if q < 2 else spot(of, y + j, z + i)

    def copy(q, what, target):
        at = buf.at[what, q]
        return pltpu.make_async_remote_copy(
            src_ref=at, dst_ref=at, send_sem=send_sem.at[len(sent)], recv_sem=recv_sem.at[what, q],
            device_id={"dp": target}, device_id_type=MESH,
        )

    def send(q, what, target):
        out = copy(q, what, target)
        out.start()
        sent.append(out)

    def take(q, i, j, to=()):
        what = piece(q, i, j)
        if (i, j) != (0, 0):
            copy(q, what, me).wait_recv()
        for target in to:
            send(q, what, piece(q, *target))
        send(q, what, spot(1 - side, y, z))

    both = ((0, 1), (0, -1))
    for q in range(4):
        take(q, 0, 0, ((1, 0), (-1, 0)) + both)
    stages = (
        (lambda d: (-d, 0), lambda d: ((d, 0),) + both),
        (lambda d: (d, 0), lambda d: both),
        (lambda d: (0, -d), lambda d: ((0, d),)),
        (lambda d: (0, d), lambda d: ()),
        (lambda d: (2, 0), lambda d: both),
        (lambda d: (-d, -d), lambda d: ((0, d),)),
        (lambda d: (d, -d), lambda d: ((0, d),)),
        (lambda d: (-d, d), lambda d: ()),
        (lambda d: (d, d), lambda d: ()),
        (lambda d: (0, 2), lambda d: ()),
        (lambda d: (2, -d), lambda d: ((0, d),)),
        (lambda d: (-d, 2), lambda d: ()),
        (lambda d: (d, 2), lambda d: ()),
        (lambda d: (2, d), lambda d: ()),
        (lambda d: (2, 2), lambda d: ()),
    )
    for where, to in stages:
        for q in range(4):
            d = 1 - 2 * (q % 2)
            take(q, *where(d), to(d))
    for i in range(RING):
        for j in range(RING):
            for q in range(4):
                copy(q, spot(1 - side, i, j), me).wait_recv()
    for out in sent:
        out.wait_send()


def torus_sems():
    n = lax.axis_size("dp")
    dma = pltpu.SemaphoreType.DMA
    return [dma((124,)), dma((n, 4))]


def near_barrier():
    side, y, z = place()
    barrier = pltpu.get_barrier_semaphore()
    peers = [
        spot(side, y + 1, z), spot(side, y - 1, z), spot(side, y, z + 1), spot(side, y, z - 1),
        spot(1 - side, y, z),
    ]
    for peer in peers:
        pl.semaphore_signal(barrier, inc=1, device_id={"dp": peer}, device_id_type=MESH)
    pl.semaphore_wait(barrier, len(peers))


def gather_kernel(q_ref, all_ref, own_sem, *sems):
    own = pltpu.make_async_copy(q_ref, all_ref.at[lax.axis_index("dp")], own_sem)
    own.start()
    near_barrier()
    own.wait()
    torus_gather(all_ref, *sems)


def gather_queries(queries):
    n = lax.axis_size("dp")
    return pl.pallas_call(
        gather_kernel,
        out_shape=jax.ShapeDtypeStruct((n,) + queries.shape, queries.dtype),
        in_specs=[pl.BlockSpec(memory_space=pltpu.VMEM)],
        out_specs=pl.BlockSpec(memory_space=pltpu.VMEM),
        scratch_shapes=[pltpu.SemaphoreType.DMA] + torus_sems(),
        compiler_params=pltpu.CompilerParams(collective_id=0, has_side_effects=True),
    )(queries)


def attend_kernel(
    sizes, codes, counts, totals, q_ref, k_hbm, v_hbm, code_ref, stat_ref,
    acc_ref, kbuf, vbuf, kmore, vmore, ksem, vsem, moresem,
):
    rows, max_pages, span, kv_local, blocks, code_base, unroll = sizes
    q_local, head_dim = q_ref.shape[1:]
    per = 128 // span
    held = per * PRE
    b = pl.program_id(0)
    f32 = jnp.float32

    def issue(block, slot):
        @pl.loop(0, rows)
        def _(r):
            row = block * rows + r

            @pl.loop(0, jnp.minimum(counts[row], held))
            def _(s):
                page = lax.div(codes[row * max_pages + s], code_base)
                pltpu.make_async_copy(k_hbm.at[page], kbuf.at[slot, r * held + s], ksem.at[slot]).start()
                pltpu.make_async_copy(v_hbm.at[page], vbuf.at[slot, r * held + s], vsem.at[slot]).start()

    @pl.when(b == 0)
    def _():
        @pl.loop(0, DEPTH)
        def _(slot):
            @pl.loop(0, rows)
            def _(r):
                vbuf[slot, pl.ds(r * held, held)] = jnp.zeros((held, span, head_dim), vbuf.dtype)

        vmore[...] = jnp.zeros(vmore.shape, vmore.dtype)
        for first in range(min(DEPTH - 1, blocks)):
            issue(first, first)

    @pl.when(b + DEPTH - 1 < blocks)
    def _():
        issue(b + DEPTH - 1, lax.rem(b + DEPTH - 1, DEPTH))

    slot = lax.rem(b, DEPTH)
    total = totals[b]
    for bit in range((rows * held).bit_length()):
        size = 1 << bit
        if size > min(rows * held, k_hbm.shape[0]):
            break

        @pl.when((total >> bit) & 1 == 1)
        def _():
            pltpu.make_async_copy(k_hbm.at[pl.ds(0, size)], kbuf.at[slot, pl.ds(0, size)], ksem.at[slot]).wait()
            pltpu.make_async_copy(v_hbm.at[pl.ds(0, size)], vbuf.at[slot, pl.ds(0, size)], vsem.at[slot]).wait()

    lane = lax.broadcasted_iota(jnp.int32, (per * q_local, 128), 1)
    line = lax.broadcasted_iota(jnp.int32, (per * q_local, 128), 0)
    fits = (lane // span == line // q_local) & (
        lane % kv_local == (line % q_local) // (q_local // kv_local)
    )
    token = jnp.where(fits, (lane % span) // kv_local, code_base)
    stat_lane = lax.broadcasted_iota(jnp.int32, (q_local, 128), 1)
    scale = head_dim ** (-0.5)

    def raw_scores(r, keys):
        return lax.dot_general(
            q_ref[r], keys, (((1,), (1,)), ((), ())), preferred_element_type=f32
        ) * scale

    def chunk(r, first, scores, values):
        row = b * rows + r
        limits = [lax.rem(codes[row * max_pages + first + i], code_base) for i in range(per)]
        limit = jnp.concatenate([jnp.full((q_local, 128), x, jnp.int32) for x in limits], axis=0)
        valid = token < limit
        spread = jnp.where(valid, jnp.concatenate([scores] * per, axis=0), NEG)
        peak = jnp.max(spread, axis=1, keepdims=True)
        weights = jnp.where(valid, jnp.exp(spread - peak), 0.0)
        mass = jnp.sum(weights, axis=1, keepdims=True)
        acc = jnp.dot(weights.astype(jnp.bfloat16), values, preferred_element_type=f32)
        peak = peak.reshape(per, q_local, 1)
        top = jnp.max(peak, axis=0)
        factor = jnp.exp(peak - top[None])
        mass = jnp.sum(mass.reshape(per, q_local, 1) * factor, axis=0)
        acc = jnp.sum(acc.reshape(per, q_local, head_dim) * factor, axis=0)
        return top, mass, acc

    def put_stats(r, stats, top, mass):
        return jnp.where(stat_lane == r, top, stats[0]), jnp.where(stat_lane == r, mass, stats[1])

    def first_chunk(r, stats):
        at = pl.ds(r * held, per)
        top, mass, acc = chunk(
            r, 0, acc_ref[r], vbuf[slot, at].reshape(128, head_dim)
        )
        acc_ref[r] = acc
        return put_stats(r, stats, top, mass)

    def body(i, stats):
        for u in range(unroll):
            stats = first_chunk(i * unroll + u, stats)
        return stats

    @pl.loop(0, rows // unroll)
    def _(i):
        for u in range(unroll):
            r = i * unroll + u
            acc_ref[r] = raw_scores(r, kbuf[slot, pl.ds(r * held, per)].reshape(128, head_dim))

    empty = (jnp.full((q_local, 128), NEG, f32), jnp.zeros((q_local, 128), f32))
    stats = lax.fori_loop(0, rows // unroll, body, empty)
    stat_ref[0], stat_ref[1] = stats

    def merge(r, part):
        top, mass, acc = part
        here = stat_lane == r
        old_top = jnp.max(jnp.where(here, stat_ref[0], NEG), axis=1, keepdims=True)
        old_mass = jnp.sum(jnp.where(here, stat_ref[1], 0.0), axis=1, keepdims=True)
        new_top = jnp.maximum(old_top, top)
        old_f = jnp.exp(old_top - new_top)
        new_f = jnp.exp(top - new_top)
        acc_ref[r] = acc_ref[r] * old_f + acc * new_f
        stat_ref[0] = jnp.where(here, new_top, stat_ref[0])
        stat_ref[1] = jnp.where(here, old_mass * old_f + mass * new_f, stat_ref[1])

    @pl.loop(0, rows)
    def _(r):
        row = b * rows + r
        count = counts[row]

        @pl.when(count > per)
        def _():
            for j in range(1, PRE):
                at = pl.ds(r * held + j * per, per)
                merge(r, chunk(
                    r, j * per,
                    raw_scores(r, kbuf[slot, at].reshape(128, head_dim)),
                    vbuf[slot, at].reshape(128, head_dim),
                ))

            @pl.loop(PRE, jnp.maximum((count + per - 1) // per, PRE))
            def _(j):
                @pl.loop(0, jnp.minimum(count - j * per, per))
                def _(s):
                    page = lax.div(codes[row * max_pages + j * per + s], code_base)
                    first = pltpu.make_async_copy(k_hbm.at[page], kmore.at[s], moresem.at[0])
                    second = pltpu.make_async_copy(v_hbm.at[page], vmore.at[s], moresem.at[1])
                    first.start()
                    second.start()
                    first.wait()
                    second.wait()

                merge(r, chunk(
                    r, j * per, raw_scores(r, kmore[...].reshape(128, head_dim)),
                    vmore[...].reshape(128, head_dim),
                ))

    def encode(i, steps):
        for u in range(unroll):
            r = i * unroll + u
            acc = acc_ref[r]
            step = jnp.max(jnp.abs(acc), axis=1, keepdims=True) * (1.0 / 32767.0)
            floor = jnp.maximum(step, 1e-30)
            inverse = 1.0 / floor
            inverse = jnp.where(step > 1e-30, inverse * (2.0 - floor * inverse), 0.0)
            code_ref[r] = jnp.round(acc * inverse).astype(jnp.int32).astype(jnp.int16)
            steps = jnp.where(stat_lane == r, step, steps)
        return steps

    stat_ref[2] = lax.fori_loop(0, rows // unroll, encode, jnp.zeros((q_local, 128), f32))


def attend(codes, counts, totals, all_queries, keys, values, page_len, kv_local, code_base, max_pages):
    blocks, rows, q_local, head_dim = all_queries.shape
    span = page_len * kv_local
    per = 128 // span
    held = per * PRE
    unroll = 32 if rows % 32 == 0 else 1
    sizes = (rows, max_pages, span, kv_local, blocks, code_base, unroll)
    return pl.pallas_call(
        functools.partial(attend_kernel, sizes),
        out_shape=(
            jax.ShapeDtypeStruct((blocks, rows, q_local, head_dim), jnp.int16),
            jax.ShapeDtypeStruct((blocks, 3, q_local, 128), jnp.float32),
        ),
        grid_spec=pltpu.PrefetchScalarGridSpec(
            num_scalar_prefetch=3,
            grid=(blocks,),
            in_specs=[
                pl.BlockSpec((None, rows, q_local, head_dim), lambda b, *_: (b, 0, 0, 0)),
                pl.BlockSpec(memory_space=pl.ANY),
                pl.BlockSpec(memory_space=pl.ANY),
            ],
            out_specs=(
                pl.BlockSpec((None, rows, q_local, head_dim), lambda b, *_: (b, 0, 0, 0)),
                pl.BlockSpec((None, 3, q_local, 128), lambda b, *_: (b, 0, 0, 0)),
            ),
            scratch_shapes=[
                pltpu.VMEM((rows, q_local, head_dim), jnp.float32),
                pltpu.VMEM((DEPTH, rows * held, span, head_dim), keys.dtype),
                pltpu.VMEM((DEPTH, rows * held, span, head_dim), keys.dtype),
                pltpu.VMEM((per, span, head_dim), keys.dtype),
                pltpu.VMEM((per, span, head_dim), keys.dtype),
                pltpu.SemaphoreType.DMA((DEPTH,)),
                pltpu.SemaphoreType.DMA((DEPTH,)),
                pltpu.SemaphoreType.DMA((2,)),
            ],
        ),
        compiler_params=pltpu.CompilerParams(dimension_semantics=("arbitrary",)),
    )(codes, counts, totals, all_queries, keys, values)


def finish_kernel(
    acc_hbm, stat_hbm, w_hbm, att_out, proj_out,
    got_acc, got_stat, weight, mixed, everyone, part, got_pair, summed, got_part,
    acc_send, acc_recv, stat_send, stat_recv, own_sem, w_sem,
    pair_send, pair_recv, part_send, part_recv,
    torus_send, torus_recv,
):
    n = lax.axis_size("dp")
    me = lax.axis_index("dp")
    m = lax.axis_size("mp")
    mine = lax.axis_index("mp")
    rows, q_local, head_dim = att_out.shape
    out_rows = proj_out.shape[0]
    pieces = pair_send.shape[0]
    width = proj_out.shape[1] // pieces
    load_w = pltpu.make_async_copy(w_hbm, weight, w_sem)
    load_w.start()
    own_acc = pltpu.make_async_copy(acc_hbm.at[me], got_acc.at[0], own_sem.at[0])
    own_stat = pltpu.make_async_copy(stat_hbm.at[me], got_stat.at[0], own_sem.at[1])
    own_acc.start()
    own_stat.start()
    axis_barrier(("dp", "mp"))

    stat_copies, acc_copies = [None], [None]
    for step in range(1, n):
        peer = lax.rem(me + step, n)
        for src, dst, send, recv, copies in (
            (stat_hbm, got_stat, stat_send, stat_recv, stat_copies),
            (acc_hbm, got_acc, acc_send, acc_recv, acc_copies),
        ):
            copies.append(pltpu.make_async_remote_copy(
                src_ref=src.at[peer], dst_ref=dst.at[step],
                send_sem=send.at[step], recv_sem=recv.at[step],
                device_id={"dp": peer}, device_id_type=MESH,
            ))
    for copies in (stat_copies, acc_copies):
        for copy in copies[1:]:
            copy.start()
    own_stat.wait()
    for copy in stat_copies[1:]:
        copy.wait()

    top = got_stat[0, 0]
    for s in range(1, n):
        top = jnp.maximum(top, got_stat[s, 0])
    factors = [jnp.exp(got_stat[s, 0] - top) for s in range(n)]
    mass = factors[0] * got_stat[0, 1]
    for s in range(1, n):
        mass = mass + factors[s] * got_stat[s, 1]
    gains = [factors[s] * got_stat[s, 2] / mass for s in range(n)]
    own_acc.wait()
    for s in range(n):
        if s:
            acc_copies[s].wait()
        for r in range(rows):
            term = gains[s][:, r : r + 1] * got_acc[s, r].astype(jnp.float32)
            mixed[r] = mixed[r] + term if s else term
    att_out[...] = mixed[...].astype(jnp.bfloat16)
    for h in range(q_local):
        at = (h % 4) * head_dim
        everyone[me, h // 4, :, at : at + head_dim] = mixed[:, h, :].astype(jnp.bfloat16)

    torus_gather(everyone, torus_send, torus_recv)
    load_w.wait()

    pair = lax.rem(mine, 2)
    group = mine // 2
    groups = m // 2

    def pair_copy(piece):
        return pltpu.make_async_remote_copy(
            src_ref=part.at[piece, :, 1 - pair], dst_ref=got_pair.at[piece],
            send_sem=pair_send.at[piece], recv_sem=pair_recv.at[piece],
            device_id={"mp": group * 2 + 1 - pair}, device_id_type=MESH,
        )

    def group_copy(piece, step):
        return pltpu.make_async_remote_copy(
            src_ref=summed.at[piece, step], dst_ref=got_part.at[piece, step],
            send_sem=part_send.at[step, piece], recv_sem=part_recv.at[step, piece],
            device_id={"mp": lax.rem(group + step, groups) * 2 + pair}, device_id_type=MESH,
        )

    band = q_local * head_dim // 4
    for piece in range(pieces):
        value = 0.0
        for q in range(4):
            value += jnp.dot(
                everyone[:, q].reshape(n * rows, band),
                weight[q * band : (q + 1) * band, piece * width : (piece + 1) * width],
                preferred_element_type=jnp.float32,
            )
        part[piece] = value.reshape(groups, 2, out_rows, width)
        pair_copy(piece).start()
    for piece in range(pieces):
        pair_copy(piece).wait()
        for step in range(groups):
            at = lax.rem(group + step, groups)
            summed[piece, step] = part[piece, at, pair] + got_pair[piece, at]
        for step in range(1, groups):
            group_copy(piece, step).start()
    for piece in range(pieces):
        total = summed[piece, 0]
        for step in range(1, groups):
            group_copy(piece, step).wait()
            total = total + got_part[piece, step]
        proj_out[:, piece * width : (piece + 1) * width] = total.astype(jnp.bfloat16)


def finish(acc, stat, out_weight):
    n, rows, q_local, head_dim = acc.shape
    m = lax.axis_size("mp")
    depth, columns = out_weight.shape
    out_rows = n * rows // m
    pieces = max(columns // 256, 1)
    width = columns // pieces
    dma = pltpu.SemaphoreType.DMA
    return pl.pallas_call(
        finish_kernel,
        out_shape=(
            jax.ShapeDtypeStruct((rows, q_local, head_dim), jnp.bfloat16),
            jax.ShapeDtypeStruct((out_rows, columns), jnp.bfloat16),
        ),
        in_specs=[pl.BlockSpec(memory_space=pl.ANY)] * 3,
        out_specs=(pl.BlockSpec(memory_space=pltpu.VMEM),) * 2,
        scratch_shapes=[
            pltpu.VMEM((n, rows, q_local, head_dim), acc.dtype),
            pltpu.VMEM((n, 3, q_local, 128), jnp.float32),
            pltpu.VMEM((depth, columns), out_weight.dtype),
            pltpu.VMEM((rows, q_local, head_dim), jnp.float32),
            pltpu.VMEM((n, 4, rows, q_local * head_dim // 4), jnp.bfloat16),
            pltpu.VMEM((pieces, m // 2, 2, out_rows, width), jnp.float32),
            pltpu.VMEM((pieces, m // 2, out_rows, width), jnp.float32),
            pltpu.VMEM((pieces, m // 2, out_rows, width), jnp.float32),
            pltpu.VMEM((pieces, m // 2, out_rows, width), jnp.float32),
            dma((n,)), dma((n,)), dma((n,)), dma((n,)), dma((2,)), dma,
            dma((pieces,)), dma((pieces,)), dma((m // 2, pieces)), dma((m // 2, pieces)),
        ] + torus_sems(),
        compiler_params=pltpu.CompilerParams(collective_id=1, has_side_effects=True),
    )(acc, stat, out_weight)


def shards(queries, lookup_sheets, content_sheets, page_table, context_len, out_weight):
    req_rows, max_pages = page_table.shape
    pool_local, page_len, kv_local, head_dim = lookup_sheets.shape
    dp_count = lax.axis_size("dp")
    rows_mine = req_rows // dp_count
    code_base = 2 * page_len
    span = page_len * kv_local
    held = (128 // span) * PRE

    local = page_table - lax.axis_index("dp") * pool_local
    slots = jnp.arange(max_pages, dtype=jnp.int32)
    used = jnp.clip(context_len[:, None] - slots[None, :] * page_len, 0, page_len)
    wanted = (local >= 0) & (local < pool_local) & (used > 0)
    before = (slots[:, None] < slots[None, :]).astype(jnp.bfloat16)
    rank = jnp.dot(
        wanted.astype(jnp.bfloat16), before, preferred_element_type=jnp.float32
    ).astype(jnp.int32)
    code = jnp.where(wanted, local * code_base + used, 0)
    rank = jnp.where(wanted, rank, -1)
    codes = jnp.sum(
        jnp.where(rank[:, None, :] == slots[None, :, None], code[:, None, :], 0), axis=2
    )
    counts = jnp.sum(wanted.astype(jnp.int32), axis=1)
    totals = jnp.sum(jnp.minimum(counts, held).reshape(dp_count, rows_mine), axis=1)

    all_queries = gather_queries(queries.reshape(4, rows_mine // 4, *queries.shape[1:]))
    all_queries = all_queries.reshape(dp_count, *queries.shape)
    acc, stat = attend(
        codes.reshape(-1), counts, totals, all_queries,
        lookup_sheets.reshape(pool_local, span, head_dim),
        content_sheets.reshape(pool_local, span, head_dim),
        page_len, kv_local, code_base, max_pages,
    )
    return finish(acc, stat, out_weight)


def solution(mesh):
    placed = (
        P("dp", "mp", None),
        P("dp", None, "mp", None),
        P("dp", None, "mp", None),
        P(),
        P(),
        P("mp", "dp"),
    )
    return jax.shard_map(
        shards,
        mesh=mesh,
        in_specs=placed,
        out_specs=(P("dp", "mp", None), P("mp", "dp")),
        check_vma=False,
    )
```

```python
import functools

import jax
import jax.numpy as jnp
from jax import lax
from jax.experimental import pallas as pl
from jax.experimental.pallas import tpu as pltpu
from jax.sharding import PartitionSpec as P

MESH = pl.DeviceIdType.MESH
NEG = -1e30
RING = 4
LISTED = 2048
GROUP = 4
UNROLL = 4


def place():
    me = lax.axis_index("dp")
    return lax.rem(me, 2), lax.rem(me // 2, RING), me // (2 * RING)


def around(i):
    return lax.rem(i + RING, RING)


def spot(side, y, z):
    return (around(z) * RING + around(y)) * 2 + side


def remote(src, dst, send, recv, target):
    return pltpu.make_async_remote_copy(
        src_ref=src, dst_ref=dst, send_sem=send, recv_sem=recv,
        device_id=target, device_id_type=MESH,
    )


def greet(peers):
    barrier = pltpu.get_barrier_semaphore()
    for peer in peers:
        pl.semaphore_signal(barrier, inc=1, device_id=peer, device_id_type=MESH)
    pl.semaphore_wait(barrier, len(peers))


def near():
    side, y, z = place()
    return [
        {"dp": spot(side, y + 1, z)}, {"dp": spot(side, y - 1, z)},
        {"dp": spot(side, y, z + 1)}, {"dp": spot(side, y, z - 1)},
        {"dp": spot(1 - side, y, z)},
    ]


def torus_gather(view, send_sem, recv_sem, filler=None):
    side, y, z = place()
    sent = []

    def piece(q, i, j):
        return (side, y + i, z + j) if q < 2 else (side, y + j, z + i)

    def copy(q, what, target):
        at = view(q, *what)
        return remote(at, at, send_sem.at[len(sent)], recv_sem.at[spot(*what), q], {"dp": target})

    def send(q, what, target):
        out = copy(q, what, target)
        out.start()
        sent.append(out)

    def take(q, i, j, to=()):
        what = piece(q, i, j)
        if (i, j) != (0, 0):
            copy(q, what, spot(side, y, z)).wait_recv()
        for target in to:
            send(q, what, spot(*piece(q, *target)))
        send(q, what, spot(1 - side, y, z))

    both = ((0, 1), (0, -1))
    for q in range(4):
        take(q, 0, 0, ((1, 0), (-1, 0)) + both)
    if filler is not None:
        filler()
    stages = (
        (lambda d: (-d, 0), lambda d: ((d, 0),) + both),
        (lambda d: (d, 0), lambda d: both),
        (lambda d: (0, -d), lambda d: ((0, d),)),
        (lambda d: (0, d), lambda d: ()),
        (lambda d: (2, 0), lambda d: both),
        (lambda d: (-d, -d), lambda d: ((0, d),)),
        (lambda d: (d, -d), lambda d: ((0, d),)),
        (lambda d: (-d, d), lambda d: ()),
        (lambda d: (d, d), lambda d: ()),
        (lambda d: (0, 2), lambda d: ()),
        (lambda d: (2, -d), lambda d: ((0, d),)),
        (lambda d: (-d, 2), lambda d: ()),
        (lambda d: (d, 2), lambda d: ()),
        (lambda d: (2, d), lambda d: ()),
        (lambda d: (2, 2), lambda d: ()),
    )
    for where, to in stages:
        for q in range(4):
            d = 1 - 2 * (q % 2)
            take(q, *where(d), to(d))
    for i in range(RING):
        for j in range(RING):
            for q in range(4):
                copy(q, (1 - side, i, j), spot(side, y, z)).wait_recv()
    for out in sent:
        out.wait_send()


def torus_sems():
    n = lax.axis_size("dp")
    dma = pltpu.SemaphoreType.DMA
    return [dma((124,)), dma((n, 4))]


def plan(sizes, table_ref, len_ref, list_ref, pos_ref, code_ref):
    pool_local, page_len = sizes
    slots, rows = table_ref.shape
    f32, bf16, i32 = jnp.float32, jnp.bfloat16, jnp.int32

    def iota(shape, dim):
        return lax.broadcasted_iota(i32, shape, dim)

    def ones(mask):
        return jnp.where(mask, 1.0, 0.0)

    local = table_ref[...] - lax.axis_index("dp") * pool_local
    used = jnp.clip(len_ref[...] - iota((slots, rows), 0) * page_len, 0, page_len)
    wanted = (local >= 0) & (local < pool_local) & (used > 0)
    flags = ones(wanted)
    lower = ones(iota((slots, slots), 1) < iota((slots, slots), 0)).astype(bf16)
    rank = jnp.dot(lower, flags.astype(bf16), preferred_element_type=f32)
    count = jnp.sum(flags, axis=0, keepdims=True)
    some = jnp.minimum(count, 1.0)
    extra = jnp.maximum(count - 1.0, 0.0)
    both = jnp.where(iota((8, rows), 0) == 0, some, extra).astype(bf16)
    upper = ones(iota((rows, rows), 0) < iota((rows, rows), 1)).astype(bf16)
    ahead = jnp.dot(both, upper, preferred_element_type=f32)
    pos = jnp.where(rank == 0.0, ahead[0:1], (LISTED - 1) - ahead[1:2] - (rank - 1.0))
    pos_ref[...] = jnp.where(wanted, pos, -1.0).astype(i32)

    t = iota((1, rows), 1)
    q, turn, y, z = (t >> 3) & 3, (t >> 5) & 1, (t >> 6) & 3, (t >> 8) & 3
    f = jnp.where(q < 2, y, z)
    g = jnp.where(q < 2, z, y)
    row = (q << 8) | (f << 6) | (turn << 5) | (g << 3) | (t & 7)
    code_ref[...] = jnp.where(wanted, (row << 15) | (local << 5) | used, 0)

    high = iota((LISTED // 128, rows), 0)
    low = iota((128, rows), 0)

    def collect(s, total):
        p = pos_ref[pl.ds(s, 1)]
        c = code_ref[pl.ds(s, 1)]
        hit = high == (p >> 7)
        bytes_of = [jnp.where(hit, ((c >> (8 * k)) & 255).astype(f32), 0.0) for k in range(4)]
        left = jnp.concatenate(bytes_of, axis=0).astype(bf16)
        right = ones(low == (p & 127)).astype(bf16)
        return total + lax.dot_general(
            left, right, (((1,), (1,)), ((), ())), preferred_element_type=f32
        )

    height = LISTED // 128
    total = lax.fori_loop(0, slots, collect, jnp.zeros((4 * height, 128), f32)).astype(i32)
    out = total[:height]
    for k in range(1, 4):
        out = out + total[k * height : (k + 1) * height] * (1 << (8 * k))
    list_ref[0:height] = jnp.where(out == 0, rows << 15, out)
    sums = jnp.where(
        iota((8, 128), 0) == 0, jnp.sum(some, axis=1, keepdims=True),
        jnp.sum(extra, axis=1, keepdims=True),
    )
    list_ref[height : height + 8] = sums.astype(i32)


def gather_kernel(
    sizes, q_ref, table_ref, len_ref, all_ref, list_ref, pos_ref, code_ref, own_sem, send, recv
):
    side, y, z = place()

    def view(q, of, at_y, at_z):
        f, g = (at_y, at_z) if q < 2 else (at_z, at_y)
        return all_ref.at[q, around(f), of, around(g)]

    own = [
        pltpu.make_async_copy(q_ref.at[q], view(q, side, y, z), own_sem.at[q]) for q in range(4)
    ]
    for copy in own:
        copy.start()
    greet(near())
    for copy in own:
        copy.wait()
    torus_gather(
        view, send, recv,
        lambda: plan(sizes, table_ref, len_ref, list_ref, pos_ref, code_ref),
    )


def gather_queries(queries, table, lengths, sizes):
    rows, q_local, head_dim = queries.shape
    dma = pltpu.SemaphoreType.DMA
    vmem = pl.BlockSpec(memory_space=pltpu.VMEM)
    return pl.pallas_call(
        functools.partial(gather_kernel, sizes),
        out_shape=(
            jax.ShapeDtypeStruct((4, RING, 2, RING, rows // 4, q_local, head_dim), queries.dtype),
            jax.ShapeDtypeStruct((LISTED // 128 + 8, 128), jnp.int32),
        ),
        in_specs=[vmem] * 3,
        out_specs=(vmem, vmem),
        scratch_shapes=[
            pltpu.VMEM(table.shape, jnp.int32), pltpu.VMEM(table.shape, jnp.int32), dma((4,)),
        ] + torus_sems(),
        compiler_params=pltpu.CompilerParams(collective_id=0, has_side_effects=True),
    )(queries.reshape(4, rows // 4, q_local, head_dim), table, lengths)


def attend_kernel(sizes, listed, q_ref, k_hbm, v_hbm, acc_ref, stat_ref, kbuf, vbuf, sem):
    kv_local, blocks = sizes
    rows, q_local, head_dim = q_ref.shape
    pages, span, _ = k_hbm.shape
    f32, i32 = jnp.float32, jnp.int32
    tall = GROUP * q_local
    wide = GROUP * span
    loads = []
    for src, dst, i in ((k_hbm, kbuf, 0), (v_hbm, vbuf, 1)):
        loads.append(pltpu.make_async_copy(src, dst, sem.at[i]))
    for load in loads:
        load.start()

    @pl.loop(0, blocks)
    def _(b):
        acc_ref[b] = jnp.zeros(acc_ref.shape[1:], f32)
        stat_ref[b, 0] = jnp.full((q_local, 128), NEG, f32)
        stat_ref[b, 1] = jnp.zeros((q_local, 128), f32)

    for load in loads:
        load.wait()

    lane = lax.broadcasted_iota(i32, (tall, wide), 1)
    line = lax.broadcasted_iota(i32, (tall, wide), 0)
    fits = (lane // span == line // q_local) & (
        lane % kv_local == (line % q_local) // (q_local // kv_local)
    )
    token = jnp.where(fits, (lane % span) // kv_local, 64)
    stat_lane = lax.broadcasted_iota(i32, (q_local, 128), 1)
    scale = head_dim ** (-0.5)
    in_block = rows // (blocks - 1)

    def chunk(first):
        codes = [listed[first + i] for i in range(GROUP)]
        used = [code & 31 for code in codes]
        page = [(code >> 5) & (pages - 1) for code in codes]
        row = [code >> 15 for code in codes]
        asked = jnp.concatenate([q_ref[r & (rows - 1)] for r in row], axis=0)
        keys = jnp.concatenate([kbuf[p] for p in page], axis=0)
        values = jnp.concatenate([vbuf[p] for p in page], axis=0)
        scores = lax.dot_general(
            asked, keys, (((1,), (1,)), ((), ())), preferred_element_type=f32
        ) * scale
        limit = jnp.concatenate([jnp.full((q_local, wide), u, i32) for u in used], axis=0)
        valid = token < limit
        scores = jnp.where(valid, scores, NEG)
        peak = jnp.max(scores, axis=1, keepdims=True)
        weights = jnp.where(valid, jnp.exp(scores - peak), 0.0)
        mass = jnp.sum(weights, axis=1, keepdims=True)
        acc = jnp.dot(weights.astype(jnp.bfloat16), values, preferred_element_type=f32)
        return [
            (row[i], peak[i * q_local : (i + 1) * q_local], mass[i * q_local : (i + 1) * q_local],
             acc[i * q_local : (i + 1) * q_local])
            for i in range(GROUP)
        ]

    first_count = listed[LISTED]
    more_count = listed[LISTED + 128]
    step = GROUP * UNROLL

    @pl.loop(0, (first_count + step - 1) // step)
    def _(i):
        parts = []
        for u in range(UNROLL):
            parts += chunk(i * step + u * GROUP)
        for row, peak, mass, acc in parts:
            block, at = row // in_block, lax.rem(row, in_block)
            here = stat_lane == at
            acc_ref[block, at] = acc
            stat_ref[block, 0] = jnp.where(here, peak, stat_ref[block, 0])
            stat_ref[block, 1] = jnp.where(here, mass, stat_ref[block, 1])

    @pl.loop(0, (more_count + GROUP - 1) // GROUP)
    def _(i):
        for row, peak, mass, acc in chunk(LISTED - GROUP - i * GROUP):
            block, at = row // in_block, lax.rem(row, in_block)
            here = stat_lane == at
            old_peak = jnp.max(jnp.where(here, stat_ref[block, 0], NEG), axis=1, keepdims=True)
            old_mass = jnp.sum(jnp.where(here, stat_ref[block, 1], 0.0), axis=1, keepdims=True)
            top = jnp.maximum(old_peak, peak)
            old_f = jnp.exp(old_peak - top)
            new_f = jnp.exp(peak - top)
            acc_ref[block, at] = acc_ref[block, at] * old_f + acc * new_f
            stat_ref[block, 0] = jnp.where(here, top, stat_ref[block, 0])
            stat_ref[block, 1] = jnp.where(here, old_mass * old_f + mass * new_f, stat_ref[block, 1])


def attend(listed, queries, keys, values, kv_local):
    rows, q_local, head_dim = queries.shape
    blocks = rows // 32 + 1
    vmem = pl.BlockSpec(memory_space=pltpu.VMEM)
    hbm = pl.BlockSpec(memory_space=pl.ANY)
    return pl.pallas_call(
        functools.partial(attend_kernel, (kv_local, blocks)),
        out_shape=(
            jax.ShapeDtypeStruct((blocks, 32, q_local, head_dim), jnp.float32),
            jax.ShapeDtypeStruct((blocks, 2, q_local, 128), jnp.float32),
        ),
        in_specs=[pl.BlockSpec(memory_space=pltpu.SMEM), vmem, hbm, hbm],
        out_specs=(vmem, vmem),
        scratch_shapes=[
            pltpu.VMEM(keys.shape, keys.dtype),
            pltpu.VMEM(values.shape, values.dtype),
            pltpu.SemaphoreType.DMA((2,)),
        ],
    )(listed, queries, keys, values)


def finish_kernel(
    acc_hbm, stat_hbm, w_hbm, att_out, proj_out,
    own_acc, own_stat, got_acc, got_stat, out_code, out_stat, in_code, in_stat,
    last_code, last_stat, weight, mixed, everyone, part, got_pair, summed, got_part,
    own_sem, cross_send, cross_recv, hop_send, hop_recv, last_send, last_recv, w_sem,
    pair_send, pair_recv, part_send, part_recv,
    torus_send, torus_recv,
):
    n = lax.axis_size("dp")
    me = lax.axis_index("dp")
    m = lax.axis_size("mp")
    mine = lax.axis_index("mp")
    side, y, z = place()
    rows, q_local, head_dim = att_out.shape
    out_rows = proj_out.shape[0]
    pieces = pair_send.shape[0]
    width = proj_out.shape[1] // pieces
    f32 = jnp.float32
    load_w = pltpu.make_async_copy(w_hbm, weight, w_sem)
    load_w.start()

    def axes(q):
        return jnp.where(q < 2, y, z), jnp.where(q < 2, z, y), 1 - 2 * lax.rem(q, 2)

    def first_axis(q, i):
        return {"dp": jnp.where(q < 2, spot(side, y + i, z), spot(side, y, z + i))}

    def second_axis(q, i):
        return {"dp": jnp.where(q < 2, spot(side, y, z + i), spot(side, y + i, z))}

    def block_of(kind, q, of):
        f, _, d = axes(q)
        f = around(f + jnp.where(kind == 0, 2, jnp.where(kind == 1, -d, jnp.where(kind == 2, d, 0))))
        return (q * RING + f) * 2 + of

    def own_copies(kind, q):
        at = block_of(kind, q, side)
        return (
            pltpu.make_async_copy(acc_hbm.at[at], own_acc.at[kind, q], own_sem.at[0, kind, q]),
            pltpu.make_async_copy(stat_hbm.at[at], own_stat.at[kind, q], own_sem.at[1, kind, q]),
        )

    def cross_copies(kind, q):
        at = block_of(kind, q, 1 - side)
        peer = {"dp": spot(1 - side, y, z)}
        return (
            remote(acc_hbm.at[at], got_acc.at[kind, q], cross_send.at[0, kind, q],
                   cross_recv.at[0, kind, q], peer),
            remote(stat_hbm.at[at], got_stat.at[kind, q], cross_send.at[1, kind, q],
                   cross_recv.at[1, kind, q], peer),
        )

    def hop_copies(kind, q):
        _, _, d = axes(q)
        peer = first_axis(q, jnp.where(kind == 1, -d, d))
        return (
            remote(out_code.at[kind, q], in_code.at[kind, q], hop_send.at[0, kind, q],
                   hop_recv.at[0, kind, q], peer),
            remote(out_stat.at[kind, q], in_stat.at[kind, q], hop_send.at[1, kind, q],
                   hop_recv.at[1, kind, q], peer),
        )

    eighth = rows // 4

    def last_copies(o, q):
        _, g, _ = axes(q)
        peer = second_axis(q, o)
        return (
            remote(out_code.at[3, q, pl.ds(around(g + o) * eighth, eighth)], last_code.at[o - 1, q],
                   last_send.at[0, o - 1, q], last_recv.at[0, o - 1, q], peer),
            remote(out_stat.at[3, q], last_stat.at[o - 1, q],
                   last_send.at[1, o - 1, q], last_recv.at[1, o - 1, q], peer),
        )

    @pl.loop(0, 16)
    def _(i):
        for copy in own_copies(i // 4, lax.rem(i, 4)):
            copy.start()

    peers = near() + [{"dp": spot(side, y + 2, z)}, {"dp": spot(side, y, z + 2)}]
    peers += [{"mp": lax.rem(mine + i, m)} for i in range(1, m)]
    greet(peers)

    @pl.loop(0, 16)
    def _(i):
        for copy in cross_copies(i // 4, lax.rem(i, 4)):
            copy.start()

    stat_lane = lax.broadcasted_iota(jnp.int32, (q_local, 128), 1)

    def aside(tile, by):
        return pltpu.roll(tile, by % 128, 1)

    def combine(tops, masses, steps):
        top = tops[0]
        for other in tops[1:]:
            top = jnp.maximum(top, other)
        mass = 0.0
        gains = []
        for each, its_mass, step in zip(tops, masses, steps):
            factor = jnp.exp(each - top)
            mass = mass + factor * its_mass
            gains.append(factor if step is None else factor * step)
        return top, mass, gains

    def gathered(kind, q, arrived):
        for copy in own_copies(kind, q):
            copy.wait()
        for copy in cross_copies(kind, q):
            copy.wait_recv()
        tops = [own_stat[kind, q, 0], got_stat[kind, q, 0]]
        masses = [own_stat[kind, q, 1], got_stat[kind, q, 1]]
        steps = [None, None]
        for other in arrived:
            for copy in hop_copies(other, q):
                copy.wait_recv()
            tile = in_stat[other, q]
            tops.append(tile)
            masses.append(aside(tile, -32))
            steps.append(aside(tile, -64))
        top, mass, gains = combine(tops, masses, steps)
        step_tile = jnp.zeros((q_local, 128), f32)
        for r in range(rows):
            value = own_acc[kind, q, r] * gains[0][:, r : r + 1]
            value = value + got_acc[kind, q, r] * gains[1][:, r : r + 1]
            for k, other in enumerate(arrived):
                value = value + in_code[other, q, r].astype(f32) * gains[2 + k][:, r : r + 1]
            step = jnp.max(jnp.abs(value), axis=1, keepdims=True) * (1.0 / 32767.0)
            floor = jnp.maximum(step, 1e-30)
            inverse = 1.0 / floor
            inverse = jnp.where(step > 1e-30, inverse * (2.0 - floor * inverse), 0.0)
            out_code[kind, q, r] = jnp.round(value * inverse).astype(jnp.int32).astype(jnp.int16)
            step_tile = jnp.where(stat_lane == r, step, step_tile)
        out_stat[kind, q] = jnp.where(
            stat_lane < 32, top,
            jnp.where(stat_lane < 64, aside(mass, 32), aside(step_tile, 64)),
        )

    @pl.loop(0, 8)
    def _(i):
        kind, q = i // 4, lax.rem(i, 4)
        gathered(kind, q, ())
        for copy in hop_copies(kind, q):
            copy.start()

    @pl.loop(0, 4)
    def _(q):
        gathered(2, q, (0,))
        for copy in hop_copies(2, q):
            copy.start()

    @pl.loop(0, 4)
    def _(q):
        gathered(3, q, (1, 2))
        for o in (1, 3, 2):
            for copy in last_copies(o, q):
                copy.start()

    @pl.loop(0, 4)
    def _(q):
        _, g, _ = axes(q)
        shift = lax.rem(128 - g * eighth, 128)
        tiles = [out_stat[3, q]]
        for o in range(1, 4):
            for copy in last_copies(o, q):
                copy.wait_recv()
            tiles.append(last_stat[o - 1, q])
        tiles = [pltpu.roll(tile, shift, 1) for tile in tiles]
        _, mass, gains = combine(
            tiles, [aside(tile, -32) for tile in tiles], [aside(tile, -64) for tile in tiles]
        )
        gains = [gain / mass for gain in gains]
        for r in range(eighth):
            value = out_code[3, q, g * eighth + r].astype(f32) * gains[0][:, r : r + 1]
            for o in range(1, 4):
                value = value + last_code[o - 1, q, r].astype(f32) * gains[o][:, r : r + 1]
            mixed[q * eighth + r] = value

    att_out[...] = mixed[...].astype(jnp.bfloat16)
    for h in range(q_local):
        at = (h % 4) * head_dim
        everyone[me, h // 4, :, at : at + head_dim] = mixed[:, h, :].astype(jnp.bfloat16)

    torus_gather(lambda q, of, at_y, at_z: everyone.at[spot(of, at_y, at_z), q], torus_send, torus_recv)
    load_w.wait()

    pair = lax.rem(mine, 2)
    group = mine // 2
    groups = m // 2

    def pair_copy(piece):
        return remote(
            part.at[piece, :, 1 - pair], got_pair.at[piece], pair_send.at[piece],
            pair_recv.at[piece], {"mp": group * 2 + 1 - pair},
        )

    def group_copy(piece, step):
        return remote(
            summed.at[piece, step], got_part.at[piece, step], part_send.at[step, piece],
            part_recv.at[step, piece], {"mp": lax.rem(group + step, groups) * 2 + pair},
        )

    band = q_local * head_dim // 4
    for piece in range(pieces):
        value = 0.0
        for q in range(4):
            value += jnp.dot(
                everyone[:, q].reshape(n * rows, band),
                weight[q * band : (q + 1) * band, piece * width : (piece + 1) * width],
                preferred_element_type=f32,
            )
        part[piece] = value.reshape(groups, 2, out_rows, width)
        pair_copy(piece).start()
    for piece in range(pieces):
        pair_copy(piece).wait()
        for step in range(groups):
            at = lax.rem(group + step, groups)
            summed[piece, step] = part[piece, at, pair] + got_pair[piece, at]
        for step in range(1, groups):
            group_copy(piece, step).start()
    for piece in range(pieces):
        total = summed[piece, 0]
        for step in range(1, groups):
            group_copy(piece, step).wait()
            total = total + got_part[piece, step]
        proj_out[:, piece * width : (piece + 1) * width] = total.astype(jnp.bfloat16)

    @pl.loop(0, 16)
    def _(i):
        for copy in cross_copies(i // 4, lax.rem(i, 4)):
            copy.wait_send()

    @pl.loop(0, 12)
    def _(i):
        kind, q = i // 4, lax.rem(i, 4)
        for copy in hop_copies(kind, q) + last_copies(kind + 1, q):
            copy.wait_send()


def finish(acc, stat, out_weight):
    _, rows, q_local, head_dim = acc.shape
    n = lax.axis_size("dp")
    m = lax.axis_size("mp")
    depth, columns = out_weight.shape
    out_rows = n * rows // m
    pieces = max(columns // 256, 1)
    width = columns // pieces
    dma = pltpu.SemaphoreType.DMA
    f32, i16 = jnp.float32, jnp.int16
    return pl.pallas_call(
        finish_kernel,
        out_shape=(
            jax.ShapeDtypeStruct((rows, q_local, head_dim), jnp.bfloat16),
            jax.ShapeDtypeStruct((out_rows, columns), jnp.bfloat16),
        ),
        in_specs=[pl.BlockSpec(memory_space=pl.ANY)] * 3,
        out_specs=(pl.BlockSpec(memory_space=pltpu.VMEM),) * 2,
        scratch_shapes=[
            pltpu.VMEM((4, 4, rows, q_local, head_dim), f32),
            pltpu.VMEM((4, 4, 2, q_local, 128), f32),
            pltpu.VMEM((4, 4, rows, q_local, head_dim), f32),
            pltpu.VMEM((4, 4, 2, q_local, 128), f32),
            pltpu.VMEM((4, 4, rows, q_local, head_dim), i16),
            pltpu.VMEM((4, 4, q_local, 128), f32),
            pltpu.VMEM((3, 4, rows, q_local, head_dim), i16),
            pltpu.VMEM((3, 4, q_local, 128), f32),
            pltpu.VMEM((3, 4, rows // 4, q_local, head_dim), i16),
            pltpu.VMEM((3, 4, q_local, 128), f32),
            pltpu.VMEM((depth, columns), out_weight.dtype),
            pltpu.VMEM((rows, q_local, head_dim), f32),
            pltpu.VMEM((n, 4, rows, q_local * head_dim // 4), jnp.bfloat16),
            pltpu.VMEM((pieces, m // 2, 2, out_rows, width), f32),
            pltpu.VMEM((pieces, m // 2, out_rows, width), f32),
            pltpu.VMEM((pieces, m // 2, out_rows, width), f32),
            pltpu.VMEM((pieces, m // 2, out_rows, width), f32),
            dma((2, 4, 4)), dma((2, 4, 4)), dma((2, 4, 4)),
            dma((2, 3, 4)), dma((2, 3, 4)), dma((2, 3, 4)), dma((2, 3, 4)), dma,
            dma((pieces,)), dma((pieces,)), dma((m // 2, pieces)), dma((m // 2, pieces)),
        ] + torus_sems(),
        compiler_params=pltpu.CompilerParams(collective_id=1, has_side_effects=True),
    )(acc, stat, out_weight)


def shards(queries, lookup_sheets, content_sheets, page_table, context_len, out_weight):
    req_rows = page_table.shape[0]
    pool_local, page_len, kv_local, head_dim = lookup_sheets.shape
    span = page_len * kv_local
    all_queries, listed = gather_queries(
        queries, page_table.T, context_len.reshape(1, req_rows), (pool_local, page_len)
    )
    acc, stat = attend(
        listed.reshape(-1), all_queries.reshape(req_rows, *queries.shape[1:]),
        lookup_sheets.reshape(pool_local, span, head_dim),
        content_sheets.reshape(pool_local, span, head_dim), kv_local,
    )
    return finish(acc, stat, out_weight)


def solution(mesh):
    placed = (
        P("dp", "mp", None),
        P("dp", None, "mp", None),
        P("dp", None, "mp", None),
        P(),
        P(),
        P("mp", "dp"),
    )
    return jax.shard_map(
        shards,
        mesh=mesh,
        in_specs=placed,
        out_specs=(P("dp", "mp", None), P("mp", "dp")),
        check_vma=False,
    )
```

```python
import functools

import jax
import jax.numpy as jnp
from jax import lax
from jax.experimental import pallas as pl
from jax.experimental.pallas import tpu as pltpu
from jax.sharding import PartitionSpec as P

MESH = pl.DeviceIdType.MESH
NEG = -1e30
RING = 4
LISTED = 2048
GROUP = 4
UNROLL = 8


def place():
    me = lax.axis_index("dp")
    return lax.rem(me, 2), lax.rem(me // 2, RING), me // (2 * RING)


def around(i):
    return lax.rem(i + RING, RING)


def spot(side, y, z):
    return (around(z) * RING + around(y)) * 2 + side


def remote(src, dst, send, recv, target):
    return pltpu.make_async_remote_copy(
        src_ref=src, dst_ref=dst, send_sem=send, recv_sem=recv,
        device_id=target, device_id_type=MESH,
    )


def greet(peers):
    barrier = pltpu.get_barrier_semaphore()
    for peer in peers:
        pl.semaphore_signal(barrier, inc=1, device_id=peer, device_id_type=MESH)
    pl.semaphore_wait(barrier, len(peers))


def near():
    side, y, z = place()
    return [
        {"dp": spot(side, y + 1, z)}, {"dp": spot(side, y - 1, z)},
        {"dp": spot(side, y, z + 1)}, {"dp": spot(side, y, z - 1)},
        {"dp": spot(1 - side, y, z)},
    ]


def torus_gather(view, send_sem, recv_sem, filler=None):
    side, y, z = place()
    sent = []

    def piece(q, i, j):
        return (side, y + i, z + j) if q < 2 else (side, y + j, z + i)

    def copy(q, what, target):
        at = view(q, *what)
        return remote(at, at, send_sem.at[len(sent)], recv_sem.at[spot(*what), q], {"dp": target})

    def send(q, what, target):
        out = copy(q, what, target)
        out.start()
        sent.append(out)

    def take(q, i, j, to=()):
        what = piece(q, i, j)
        if (i, j) != (0, 0):
            copy(q, what, spot(side, y, z)).wait_recv()
        for target in to:
            send(q, what, spot(*piece(q, *target)))
        send(q, what, spot(1 - side, y, z))

    both = ((0, 1), (0, -1))
    for q in range(4):
        take(q, 0, 0, ((1, 0), (-1, 0)) + both)
    if filler is not None:
        filler()
    stages = (
        (lambda d: (-d, 0), lambda d: ((d, 0),) + both),
        (lambda d: (d, 0), lambda d: both),
        (lambda d: (0, -d), lambda d: ((0, d),)),
        (lambda d: (0, d), lambda d: ()),
        (lambda d: (2, 0), lambda d: both),
        (lambda d: (-d, -d), lambda d: ((0, d),)),
        (lambda d: (d, -d), lambda d: ((0, d),)),
        (lambda d: (-d, d), lambda d: ()),
        (lambda d: (d, d), lambda d: ()),
        (lambda d: (0, 2), lambda d: ()),
        (lambda d: (2, -d), lambda d: ((0, d),)),
        (lambda d: (-d, 2), lambda d: ()),
        (lambda d: (d, 2), lambda d: ()),
        (lambda d: (2, d), lambda d: ()),
        (lambda d: (2, 2), lambda d: ()),
    )
    for where, to in stages:
        for q in range(4):
            d = 1 - 2 * (q % 2)
            take(q, *where(d), to(d))
    for i in range(RING):
        for j in range(RING):
            for q in range(4):
                copy(q, (1 - side, i, j), spot(side, y, z)).wait_recv()
    for out in sent:
        out.wait_send()


def torus_sems():
    n = lax.axis_size("dp")
    dma = pltpu.SemaphoreType.DMA
    return [dma((124,)), dma((n, 4))]


def plan(sizes, table_ref, len_ref, list_ref, pos_ref, code_ref):
    pool_local, page_len = sizes
    slots, rows = table_ref.shape
    f32, bf16, i32 = jnp.float32, jnp.bfloat16, jnp.int32

    def iota(shape, dim):
        return lax.broadcasted_iota(i32, shape, dim)

    def ones(mask):
        return jnp.where(mask, 1.0, 0.0)

    local = table_ref[...] - lax.axis_index("dp") * pool_local
    used = jnp.clip(len_ref[...] - iota((slots, rows), 0) * page_len, 0, page_len)
    wanted = (local >= 0) & (local < pool_local) & (used > 0)
    flags = ones(wanted)
    lower = ones(iota((slots, slots), 1) < iota((slots, slots), 0)).astype(bf16)
    rank = jnp.dot(lower, flags.astype(bf16), preferred_element_type=f32)
    count = jnp.sum(flags, axis=0, keepdims=True)
    some = jnp.minimum(count, 1.0)
    extra = jnp.maximum(count - 1.0, 0.0)
    both = jnp.where(iota((8, rows), 0) == 0, some, extra).astype(bf16)
    upper = ones(iota((rows, rows), 0) < iota((rows, rows), 1)).astype(bf16)
    ahead = jnp.dot(both, upper, preferred_element_type=f32)
    pos = jnp.where(rank == 0.0, ahead[0:1], (LISTED - 1) - ahead[1:2] - (rank - 1.0))
    pos_ref[...] = jnp.where(wanted, pos, -1.0).astype(i32)

    t = iota((1, rows), 1)
    q, turn, y, z = (t >> 3) & 3, (t >> 5) & 1, (t >> 6) & 3, (t >> 8) & 3
    f = jnp.where(q < 2, y, z)
    g = jnp.where(q < 2, z, y)
    row = (q << 8) | (f << 6) | (turn << 5) | (g << 3) | (t & 7)
    code_ref[...] = jnp.where(wanted, (row << 15) | (local << 5) | used, 0)

    high = iota((LISTED // 128, rows), 0)
    low = iota((128, rows), 0)

    def collect(s, total):
        p = pos_ref[pl.ds(s, 1)]
        c = code_ref[pl.ds(s, 1)]
        hit = high == (p >> 7)
        bytes_of = [jnp.where(hit, ((c >> (8 * k)) & 255).astype(f32), 0.0) for k in range(4)]
        left = jnp.concatenate(bytes_of, axis=0).astype(bf16)
        right = ones(low == (p & 127)).astype(bf16)
        return total + lax.dot_general(
            left, right, (((1,), (1,)), ((), ())), preferred_element_type=f32
        )

    height = LISTED // 128
    total = lax.fori_loop(0, slots, collect, jnp.zeros((4 * height, 128), f32)).astype(i32)
    out = total[:height]
    for k in range(1, 4):
        out = out + total[k * height : (k + 1) * height] * (1 << (8 * k))
    list_ref[0:height] = jnp.where(out == 0, rows << 15, out)
    sums = jnp.where(
        iota((8, 128), 0) == 0, jnp.sum(some, axis=1, keepdims=True),
        jnp.sum(extra, axis=1, keepdims=True),
    )
    list_ref[height : height + 8] = sums.astype(i32)


def gather_kernel(
    sizes, q_ref, table_ref, len_ref, all_ref, list_ref, pos_ref, code_ref, own_sem, send, recv
):
    side, y, z = place()

    def view(q, of, at_y, at_z):
        f, g = (at_y, at_z) if q < 2 else (at_z, at_y)
        return all_ref.at[q, around(f), of, around(g)]

    own = [
        pltpu.make_async_copy(q_ref.at[q], view(q, side, y, z), own_sem.at[q]) for q in range(4)
    ]
    for copy in own:
        copy.start()
    greet(near())
    for copy in own:
        copy.wait()
    torus_gather(
        view, send, recv,
        lambda: plan(sizes, table_ref, len_ref, list_ref, pos_ref, code_ref),
    )


def gather_queries(queries, table, lengths, sizes):
    rows, q_local, head_dim = queries.shape
    dma = pltpu.SemaphoreType.DMA
    vmem = pl.BlockSpec(memory_space=pltpu.VMEM)
    return pl.pallas_call(
        functools.partial(gather_kernel, sizes),
        out_shape=(
            jax.ShapeDtypeStruct((4, RING, 2, RING, rows // 4, q_local, head_dim), queries.dtype),
            jax.ShapeDtypeStruct((LISTED // 128 + 8, 128), jnp.int32),
        ),
        in_specs=[vmem] * 3,
        out_specs=(vmem, vmem),
        scratch_shapes=[
            pltpu.VMEM(table.shape, jnp.int32), pltpu.VMEM(table.shape, jnp.int32), dma((4,)),
        ] + torus_sems(),
        compiler_params=pltpu.CompilerParams(collective_id=0, has_side_effects=True, vmem_limit_bytes=8 << 20),
        cost_estimate=pl.CostEstimate(flops=20_000_000_000, bytes_accessed=8 << 20, transcendentals=0),
    )(queries.reshape(4, rows // 4, q_local, head_dim), table, lengths)


def attend_kernel(
    sizes, listed, q_ref, kbuf, vbuf, acc_turned, stat_turned,
    acc_ref, stat_ref,
):
    kv_local, blocks = sizes
    rows, q_local, head_dim = q_ref.shape
    pages, span, _ = kbuf.shape
    f32, i32 = jnp.float32, jnp.int32
    tall = GROUP * q_local
    wide = GROUP * span
    whole_lane = lax.broadcasted_iota(i32, (128, 128), 1)

    @pl.loop(0, blocks)
    def _(b):
        acc_ref[b] = jnp.zeros(acc_ref.shape[1:], f32)
        stat_ref[b] = jnp.where(whole_lane % 2 == 0, NEG, 0.0)

    lane = lax.broadcasted_iota(i32, (tall, wide), 1)
    line = lax.broadcasted_iota(i32, (tall, wide), 0)
    fits = (lane // span == line // q_local) & (
        lane % kv_local == (line % q_local) // (q_local // kv_local)
    )
    token = jnp.where(fits, (lane % span) // kv_local, 64)
    stat_lane = lax.broadcasted_iota(i32, (q_local, 128), 1)
    scale = head_dim ** (-0.5)

    def half(first):
        codes = [listed[first + i] for i in range(GROUP)]
        used = [code & 31 for code in codes]
        page = [(code >> 5) & (pages - 1) for code in codes]
        row = [code >> 15 for code in codes]
        asked = jnp.concatenate([q_ref[r & (rows - 1)] for r in row], axis=0)
        keys = jnp.concatenate([kbuf[p] for p in page], axis=0)
        values = jnp.concatenate([vbuf[p] for p in page], axis=0)
        limit = jnp.concatenate([jnp.full((q_local, wide), u, i32) for u in used], axis=0)
        return row, asked, keys, values, token < limit

    def soft(scores, valid):
        scores = jnp.where(valid, scores * scale, NEG)
        peak = jnp.max(scores, axis=1, keepdims=True)
        weights = jnp.where(valid, jnp.exp(scores - peak), 0.0)
        return peak, jnp.sum(weights, axis=1, keepdims=True), weights.astype(jnp.bfloat16)

    def quad(firsts):
        halves = [half(first) for first in firsts]
        scores = [
            lax.dot_general(h[1], h[2], (((1,), (1,)), ((), ())), preferred_element_type=f32)
            for h in halves
        ]
        soft_of = [soft(x, h[4]) for x, h in zip(scores, halves)]
        none = jnp.zeros((tall, wide), jnp.bfloat16)
        left = jnp.concatenate([
            jnp.concatenate([x[2], none] if k % 2 == 0 else [none, x[2]], axis=1)
            for k, x in enumerate(soft_of)
        ], axis=0)
        right = jnp.concatenate([
            jnp.concatenate([halves[k][3], halves[k + 1][3]], axis=0)
            for k in range(0, len(halves), 2)
        ], axis=1)
        acc = jnp.dot(left, right, preferred_element_type=f32)
        out = []
        for k in range(len(halves)):
            part = acc[k * tall : (k + 1) * tall, (k // 2) * head_dim : (k // 2 + 1) * head_dim]
            for i in range(GROUP):
                at = slice(i * q_local, (i + 1) * q_local)
                out.append((halves[k][0][i], soft_of[k][0][at], soft_of[k][1][at], part[at]))
        return out

    def split(row):
        first = pl.multiple_of((row & 7) * q_local, q_local)
        peak_here = stat_lane == ((row >> 3) & 3) * 2
        mass_here = stat_lane == ((row >> 3) & 3) * 2 + 1
        return row >> 5, row & 31, pl.ds(first, q_local), peak_here, mass_here

    first_count = listed[LISTED]
    more_count = listed[LISTED + 128]
    step = GROUP * UNROLL

    @pl.loop(0, (first_count + step - 1) // step)
    def _(i):
        parts = []
        for u in range(0, UNROLL, 4):
            parts += quad([i * step + (u + k) * GROUP for k in range(4)])
        for row, peak, mass, acc in parts:
            block, at, lines, peak_here, mass_here = split(row)
            acc_ref[block, at] = acc
            stat_ref[block, lines] = jnp.where(
                peak_here, peak, jnp.where(mass_here, mass, stat_ref[block, lines])
            )

    @pl.loop(0, (more_count + 2 * GROUP - 1) // (2 * GROUP))
    def _(i):
        parts = quad([LISTED - GROUP - i * 2 * GROUP, LISTED - 2 * GROUP - i * 2 * GROUP])
        for row, peak, mass, acc in parts:
            block, at, lines, peak_here, mass_here = split(row)
            old = stat_ref[block, lines]
            old_peak = jnp.max(jnp.where(peak_here, old, NEG), axis=1, keepdims=True)
            old_mass = jnp.sum(jnp.where(mass_here, old, 0.0), axis=1, keepdims=True)
            top = jnp.maximum(old_peak, peak)
            old_f = jnp.exp(old_peak - top)
            new_f = jnp.exp(peak - top)
            acc_ref[block, at] = acc_ref[block, at] * old_f + acc * new_f
            stat_ref[block, lines] = jnp.where(
                peak_here, top, jnp.where(mass_here, old_mass * old_f + mass * new_f, old)
            )

    eighth = 128 // q_local

    @pl.loop(0, blocks - 1)
    def _(b):
        for g in range(4):
            tile = acc_ref[b, g * eighth : (g + 1) * eighth].reshape(128, head_dim)
            acc_turned[b, g] = tile.T
        stat_turned[b] = stat_ref[b].T[:8]


def attend(listed, queries, keys, values, kv_local):
    rows, q_local, head_dim = queries.shape
    blocks = rows // 32 + 1
    f32 = jnp.float32
    vmem = pl.BlockSpec(memory_space=pltpu.VMEM)
    return pl.pallas_call(
        functools.partial(attend_kernel, (kv_local, blocks)),
        out_shape=(
            jax.ShapeDtypeStruct((blocks - 1, 4, head_dim, 128), f32),
            jax.ShapeDtypeStruct((blocks - 1, 8, 128), f32),
        ),
        in_specs=[pl.BlockSpec(memory_space=pltpu.SMEM), vmem, vmem, vmem],
        out_specs=(vmem, vmem),
        scratch_shapes=[
            pltpu.VMEM((blocks, 32, q_local, head_dim), f32),
            pltpu.VMEM((blocks, 128, 128), f32),
        ],
        compiler_params=pltpu.CompilerParams(vmem_limit_bytes=16 << 20),
    )(listed, queries, keys, values)


def finish_kernel(
    acc_hbm, stat_hbm, w_hbm, att_out, proj_out,
    got_acc, got_stat, out_code, out_stat, in_code, in_stat,
    last_code, last_stat, weight, mixed, everyone, part_out, part_step_out, part_in, part_step_in,
    cross_send, cross_recv, hop_send, hop_recv, last_send, last_recv, w_sem,
    part_send, part_recv,
    torus_send, torus_recv,
):
    n = lax.axis_size("dp")
    me = lax.axis_index("dp")
    m = lax.axis_size("mp")
    mine = lax.axis_index("mp")
    side, y, z = place()
    rows, q_local, head_dim = att_out.shape
    out_rows = proj_out.shape[0]
    half_width = proj_out.shape[1] // 2
    f32 = jnp.float32
    load_w = pltpu.make_async_copy(w_hbm, weight, w_sem)
    load_w.start()

    def axes(q):
        return jnp.where(q < 2, y, z), jnp.where(q < 2, z, y), 1 - 2 * lax.rem(q, 2)

    def first_axis(q, i):
        return {"dp": jnp.where(q < 2, spot(side, y + i, z), spot(side, y, z + i))}

    def second_axis(q, i):
        return {"dp": jnp.where(q < 2, spot(side, y, z + i), spot(side, y + i, z))}

    def block_of(kind, q, of):
        f, _, d = axes(q)
        f = around(f + jnp.where(kind == 0, 2, jnp.where(kind == 1, -d, jnp.where(kind == 2, d, 0))))
        return (q * RING + f) * 2 + of

    def cross_copies(kind, q):
        at = block_of(kind, q, 1 - side)
        peer = {"dp": spot(1 - side, y, z)}
        return (
            remote(acc_hbm.at[at], got_acc.at[kind, q], cross_send.at[0, kind, q],
                   cross_recv.at[0, kind, q], peer),
            remote(stat_hbm.at[at], got_stat.at[kind, q], cross_send.at[1, kind, q],
                   cross_recv.at[1, kind, q], peer),
        )

    def hop_copies(kind, q):
        _, _, d = axes(q)
        peer = first_axis(q, jnp.where(kind == 1, -d, d))
        return (
            remote(out_code.at[kind, q], in_code.at[kind, q], hop_send.at[0, kind, q],
                   hop_recv.at[0, kind, q], peer),
            remote(out_stat.at[kind, q], in_stat.at[kind, q], hop_send.at[1, kind, q],
                   hop_recv.at[1, kind, q], peer),
        )

    def last_copies(o, q):
        _, g, _ = axes(q)
        peer = second_axis(q, o)
        at = around(g + o)
        return (
            remote(out_code.at[3, q, at], last_code.at[o - 1, q],
                   last_send.at[0, o - 1, q], last_recv.at[0, o - 1, q], peer),
            remote(out_stat.at[3, q, at], last_stat.at[o - 1, q],
                   last_send.at[1, o - 1, q], last_recv.at[1, o - 1, q], peer),
        )

    peers = near() + [{"dp": spot(side, y + 2, z)}, {"dp": spot(side, y, z + 2)}]
    peers += [{"mp": lax.rem(mine + i, m)} for i in range(1, m)]
    greet(peers)

    @pl.loop(0, 16)
    def _(i):
        for copy in cross_copies(i // 4, lax.rem(i, 4)):
            copy.start()

    def combine(parts):
        top = parts[0][0]
        for part in parts[1:]:
            top = jnp.maximum(top, part[0])
        mass = 0.0
        gains = []
        for its_top, its_mass, step in parts:
            factor = jnp.exp(its_top - top)
            mass = mass + factor * its_mass
            gains.append(factor if step is None else factor * step)
        return top, mass, gains

    def coded(tile):
        return tile[0:1], tile[1:2], tile[2:3]

    def encode(value):
        step = jnp.max(jnp.abs(value), axis=0, keepdims=True) * (1.0 / 32767.0)
        floor = jnp.maximum(step, 1e-30)
        inverse = 1.0 / floor
        inverse = jnp.where(step > 1e-30, inverse * (2.0 - floor * inverse), 0.0)
        return jnp.round(value * inverse).astype(jnp.int32).astype(jnp.int16), step

    def gathered(kind, q, arrived):
        own = block_of(kind, q, side)
        for copy in cross_copies(kind, q):
            copy.wait_recv()
        for other in arrived:
            for copy in hop_copies(other, q):
                copy.wait_recv()
        for g in range(4):
            plain = [
                (stat[2 * g : 2 * g + 1], stat[2 * g + 1 : 2 * g + 2], None)
                for stat in (stat_hbm[own], got_stat[kind, q])
            ]
            top, mass, gains = combine(plain + [coded(in_stat[k, q, g]) for k in arrived])
            value = acc_hbm[own, g] * gains[0] + got_acc[kind, q, g] * gains[1]
            for gain, k in zip(gains[2:], arrived):
                value = value + in_code[k, q, g].astype(f32) * gain
            out_code[kind, q, g], step = encode(value)
            out_stat[kind, q, g, 0:1] = top
            out_stat[kind, q, g, 1:2] = mass
            out_stat[kind, q, g, 2:3] = step

    @pl.loop(0, 8)
    def _(i):
        kind, q = i // 4, lax.rem(i, 4)
        gathered(kind, q, ())
        for copy in hop_copies(kind, q):
            copy.start()

    @pl.loop(0, 4)
    def _(q):
        gathered(2, q, (0,))
        for copy in hop_copies(2, q):
            copy.start()

    @pl.loop(0, 4)
    def _(q):
        gathered(3, q, (1, 2))
        for o in (1, 3, 2):
            for copy in last_copies(o, q):
                copy.start()

    @pl.loop(0, 4)
    def _(q):
        _, g, _ = axes(q)
        parts = [coded(out_stat[3, q, g])]
        for o in range(1, 4):
            for copy in last_copies(o, q):
                copy.wait_recv()
            parts.append(coded(last_stat[o - 1, q]))
        _, mass, gains = combine(parts)
        value = out_code[3, q, g].astype(f32) * (gains[0] / mass)
        for o in range(1, 4):
            value = value + last_code[o - 1, q].astype(f32) * (gains[o] / mass)
        mixed[pl.ds(q * (rows // 4), rows // 4)] = value.T.reshape(rows // 4, q_local, head_dim)

    att_out[...] = mixed[...].astype(jnp.bfloat16)
    for h in range(q_local):
        at = (h % 4) * head_dim
        everyone[me, h // 4, :, at : at + head_dim] = mixed[:, h, :].astype(jnp.bfloat16)

    torus_gather(lambda q, of, at_y, at_z: everyone.at[spot(of, at_y, at_z), q], torus_send, torus_recv)
    load_w.wait()

    band = q_local * head_dim // 4
    homes = n // m

    def rows_of(i):
        at = pl.multiple_of(lax.rem(mine + i + m, m) * homes, homes)
        value = 0.0
        for q in range(4):
            value += jnp.dot(
                everyone[pl.ds(at, homes), q].reshape(out_rows, band),
                weight[q * band : (q + 1) * band], preferred_element_type=f32,
            )
        return value

    def side_copies(kind, half):
        by = 1 - 2 * half
        peer = {"mp": lax.rem(mine + (m - by if kind == 1 else by) + m, m)}
        return (
            remote(part_out.at[kind, half], part_in.at[kind, half], part_send.at[0, kind, half],
                   part_recv.at[0, kind, half], peer),
            remote(part_step_out.at[kind, half], part_step_in.at[kind, half],
                   part_send.at[1, kind, half], part_recv.at[1, kind, half], peer),
        )

    def put(kind, half, value):
        part_out[kind, half], step = encode(value)
        part_step_out[kind, half, 0:1] = step
        for copy in side_copies(kind, half):
            copy.start()

    def arrived(kind, half):
        for copy in side_copies(kind, half):
            copy.wait_recv()
        return part_in[kind, half].astype(f32) * part_step_in[kind, half, 0:1]

    halves = [slice(0, half_width), slice(half_width, 2 * half_width)]
    value = rows_of(2)
    for half in range(2):
        put(0, half, value[:, halves[half]])
    before = rows_of(-1)
    put(1, 0, before[:, halves[0]])
    after = rows_of(1)
    put(1, 1, after[:, halves[1]])
    put(2, 0, after[:, halves[0]] + arrived(0, 0))
    put(2, 1, before[:, halves[1]] + arrived(0, 1))
    value = rows_of(0)
    for half in range(2):
        total = value[:, halves[half]] + arrived(1, half) + arrived(2, half)
        proj_out[:, halves[half]] = total.astype(jnp.bfloat16)
    for kind in range(3):
        for half in range(2):
            for copy in side_copies(kind, half):
                copy.wait_send()

    @pl.loop(0, 16)
    def _(i):
        for copy in cross_copies(i // 4, lax.rem(i, 4)):
            copy.wait_send()

    @pl.loop(0, 12)
    def _(i):
        kind, q = i // 4, lax.rem(i, 4)
        for copy in hop_copies(kind, q) + last_copies(kind + 1, q):
            copy.wait_send()


def finish(acc, stat, out_weight, q_local):
    _, _, head_dim, _ = acc.shape
    rows = 4 * 128 // q_local
    n = lax.axis_size("dp")
    m = lax.axis_size("mp")
    depth, columns = out_weight.shape
    out_rows = n * rows // m
    dma = pltpu.SemaphoreType.DMA
    f32, i16 = jnp.float32, jnp.int16
    return pl.pallas_call(
        finish_kernel,
        out_shape=(
            jax.ShapeDtypeStruct((rows, q_local, head_dim), jnp.bfloat16),
            jax.ShapeDtypeStruct((out_rows, columns), jnp.bfloat16),
        ),
        in_specs=[pl.BlockSpec(memory_space=pltpu.VMEM)] * 2 + [pl.BlockSpec(memory_space=pl.ANY)],
        out_specs=(pl.BlockSpec(memory_space=pltpu.VMEM),) * 2,
        scratch_shapes=[
            pltpu.VMEM((4, 4, 4, head_dim, 128), f32),
            pltpu.VMEM((4, 4, 8, 128), f32),
            pltpu.VMEM((4, 4, 4, head_dim, 128), i16),
            pltpu.VMEM((4, 4, 4, 4, 128), f32),
            pltpu.VMEM((3, 4, 4, head_dim, 128), i16),
            pltpu.VMEM((3, 4, 4, 4, 128), f32),
            pltpu.VMEM((3, 4, head_dim, 128), i16),
            pltpu.VMEM((3, 4, 4, 128), f32),
            pltpu.VMEM((depth, columns), out_weight.dtype),
            pltpu.VMEM((rows, q_local, head_dim), f32),
            pltpu.VMEM((n, 4, rows, q_local * head_dim // 4), jnp.bfloat16),
            pltpu.VMEM((3, 2, out_rows, columns // 2), i16),
            pltpu.VMEM((3, 2, 8, columns // 2), f32),
            pltpu.VMEM((3, 2, out_rows, columns // 2), i16),
            pltpu.VMEM((3, 2, 8, columns // 2), f32),
            dma((2, 4, 4)), dma((2, 4, 4)),
            dma((2, 3, 4)), dma((2, 3, 4)), dma((2, 3, 4)), dma((2, 3, 4)), dma,
            dma((2, 3, 2)), dma((2, 3, 2)),
        ] + torus_sems(),
        compiler_params=pltpu.CompilerParams(collective_id=1, has_side_effects=True, vmem_limit_bytes=24 << 20),
    )(acc, stat, out_weight)


def shards(queries, lookup_sheets, content_sheets, page_table, context_len, out_weight):
    req_rows = page_table.shape[0]
    pool_local, page_len, kv_local, head_dim = lookup_sheets.shape
    span = page_len * kv_local
    all_queries, listed = gather_queries(
        queries, page_table.T, context_len.reshape(1, req_rows), (pool_local, page_len)
    )
    acc, stat = attend(
        listed.reshape(-1), all_queries.reshape(req_rows, *queries.shape[1:]),
        lookup_sheets.reshape(pool_local, span, head_dim),
        content_sheets.reshape(pool_local, span, head_dim), kv_local,
    )
    return finish(acc, stat, out_weight, queries.shape[1])


def solution(mesh):
    placed = (
        P("dp", "mp", None),
        P("dp", None, "mp", None),
        P("dp", None, "mp", None),
        P(),
        P(),
        P("mp", "dp"),
    )
    return jax.shard_map(
        shards,
        mesh=mesh,
        in_specs=placed,
        out_specs=(P("dp", "mp", None), P("mp", "dp")),
        check_vma=False,
    )
```

```python
import functools

import jax
import jax.numpy as jnp
from jax import lax
from jax.experimental import pallas as pl
from jax.experimental.pallas import tpu as pltpu
from jax.sharding import PartitionSpec as P

MESH = pl.DeviceIdType.MESH
NEG = -1e30
RING = 4
LISTED = 4096
SECOND = 4096
THIRD = 1536
LATER = 2080
BATCH = 32
GROUP = 4


def place():
    me = lax.axis_index("dp")
    return lax.rem(me, 2), lax.rem(me // 2, RING), me // (2 * RING)


def around(i):
    return lax.rem(i + RING, RING)


def spot(side, y, z):
    return (around(z) * RING + around(y)) * 2 + side


def remote(src, dst, send, recv, target):
    return pltpu.make_async_remote_copy(
        src_ref=src, dst_ref=dst, send_sem=send, recv_sem=recv,
        device_id=target, device_id_type=MESH,
    )


def greet(peers):
    barrier = pltpu.get_barrier_semaphore()
    for peer in peers:
        pl.semaphore_signal(barrier, inc=1, device_id=peer, device_id_type=MESH)
    pl.semaphore_wait(barrier, len(peers))


def near():
    side, y, z = place()
    return [
        {"dp": spot(side, y + 1, z)}, {"dp": spot(side, y - 1, z)},
        {"dp": spot(side, y, z + 1)}, {"dp": spot(side, y, z - 1)},
        {"dp": spot(1 - side, y, z)},
    ]


def torus_gather(view, send_sem, recv_sem, between):
    side, y, z = place()
    here = spot(side, y, z)
    sent = []

    def piece(q, i, j):
        return (side, y + i, z + j) if q < 2 else (side, y + j, z + i)

    def copy(q, what, target):
        at = view(q, *what)
        return remote(at, at, send_sem.at[len(sent)], recv_sem.at[spot(*what), q], {"dp": target})

    def send(q, at, to):
        out = copy(q, piece(q, *at), spot(*piece(q, *to)))
        out.start()
        sent.append(out)

    def take(*wheres):
        for where, to in wheres:
            for q in range(4):
                d = 1 - 2 * (q % 2)
                at = where(d)
                copy(q, piece(q, *at), here).wait_recv()
                for target in to(d):
                    send(q, at, target)

    def cross(*wheres):
        for where in wheres:
            for q in range(4):
                what = piece(q, *where(1 - 2 * (q % 2)))
                out = copy(q, what, spot(1 - side, y, z))
                out.start()
                sent.append(out)

    def plane(j):
        for i in range(RING):
            for q in range(4):
                copy(q, (1 - side, i, z + j), here).wait_recv()

    both = ((0, 1), (0, -1))
    for q in range(4):
        for to in ((1, 0), (-1, 0)):
            send(q, (0, 0), to)
    for q in range(4):
        for to in both:
            send(q, (0, 0), to)
    cross(lambda d: (0, 0))
    between(0, plane)
    near_back, near_front = lambda d: (-d, 0), lambda d: (d, 0)
    low, high = lambda d: (0, -d), lambda d: (0, d)
    take((near_back, lambda d: ((d, 0),) + both), (low, lambda d: ((0, d),)))
    take((near_front, lambda d: both), (high, lambda d: ()))
    cross(near_back, low, near_front, high)
    between(1, plane)
    far = lambda d: (2, 0)
    take((far, lambda d: both))
    corners = [lambda d: (-d, -d), lambda d: (d, -d), lambda d: (-d, d), lambda d: (d, d)]
    take((corners[0], lambda d: ((0, d),)), (corners[1], lambda d: ((0, d),)))
    over = lambda d: (0, 2)
    take((over, lambda d: ()), (corners[2], lambda d: ()), (corners[3], lambda d: ()))
    cross(far, over, *corners)
    between(2, plane)
    take((lambda d: (2, -d), lambda d: ((0, d),)))
    rest = [lambda d: (2, d), lambda d: (-d, 2), lambda d: (d, 2)]
    take(*[(where, lambda d: ()) for where in rest])
    cross(lambda d: (2, -d), *rest)
    between(3, plane)
    take((lambda d: (2, 2), lambda d: ()))
    cross(lambda d: (2, 2))
    between(4, plane)
    for out in sent:
        out.wait_send()


def torus_sems():
    n = lax.axis_size("dp")
    dma = pltpu.SemaphoreType.DMA
    return [dma((124,)), dma((n, 4))]


def plan_start(sizes, table_ref, len_ref, list_ref, pos_ref, code_ref, total_ref):
    pool_local, page_len = sizes
    slots, rows = table_ref.shape
    f32, bf16, i32 = jnp.float32, jnp.bfloat16, jnp.int32

    def iota(shape, dim):
        return lax.broadcasted_iota(i32, shape, dim)

    def ones(mask):
        return jnp.where(mask, 1.0, 0.0)

    local = table_ref[...] - lax.axis_index("dp") * pool_local
    used = jnp.clip(len_ref[...] - iota((slots, rows), 0) * page_len, 0, page_len)
    wanted = (local >= 0) & (local < pool_local) & (used > 0)
    flags = ones(wanted)
    lower = ones(iota((slots, slots), 1) < iota((slots, slots), 0)).astype(bf16)
    rank = jnp.dot(lower, flags.astype(bf16), preferred_element_type=f32)
    count = jnp.sum(flags, axis=0, keepdims=True)
    line = iota((8, rows), 0)
    held = jnp.maximum(count - line.astype(f32), 0.0)
    held = jnp.where(line < 3, jnp.minimum(held, 1.0), jnp.where(line == 3, held, 0.0))
    upper = ones(iota((rows, rows), 0) < iota((rows, rows), 1)).astype(bf16)
    ahead = jnp.dot(held.astype(bf16), upper, preferred_element_type=f32)
    pos = jnp.where(
        rank < 2.0,
        jnp.where(rank == 0.0, ahead[0:1], SECOND - 1 - ahead[1:2]),
        jnp.where(rank == 2.0, THIRD + ahead[2:3], LATER - 3 + rank + ahead[3:4]),
    )
    pos_ref[...] = jnp.where(wanted, pos, -1.0).astype(i32)

    t = iota((1, rows), 1)
    q, turn, y, z = (t >> 3) & 3, (t >> 5) & 1, (t >> 6) & 3, (t >> 8) & 3
    f = jnp.where(q < 2, y, z)
    g = jnp.where(q < 2, z, y)
    row = (q << 8) | (f << 6) | (turn << 5) | (g << 3) | (t & 7)
    code_ref[...] = jnp.where(wanted, (row << 15) | (local << 5) | used, 0)
    total_ref[...] = jnp.zeros(total_ref.shape, f32)
    height = LISTED // 128
    sums = jnp.sum(held, axis=1, keepdims=True) + jnp.zeros((8, 128), f32)
    list_ref[height : height + 8] = sums.astype(i32)


def plan_collect(first, last, pos_ref, code_ref, total_ref):
    rows = pos_ref.shape[1]
    f32, bf16, i32 = jnp.float32, jnp.bfloat16, jnp.int32
    high = lax.broadcasted_iota(i32, (LISTED // 128, rows), 0)
    low = lax.broadcasted_iota(i32, (128, rows), 0)

    def collect(s, total):
        p = pos_ref[pl.ds(s, 1)]
        c = code_ref[pl.ds(s, 1)]
        hit = high == (p >> 7)
        left = [jnp.where(hit, ((c >> (8 * k)) & 255).astype(f32), 0.0) for k in range(4)]
        left = jnp.concatenate(left, axis=0).astype(bf16)
        right = jnp.where(low == (p & 127), 1.0, 0.0).astype(bf16)
        return total + lax.dot_general(
            left, right, (((1,), (1,)), ((), ())), preferred_element_type=f32
        )

    total_ref[...] = lax.fori_loop(first, last, collect, total_ref[...])


def plan_finish(list_ref, total_ref, rows):
    height = LISTED // 128
    total = total_ref[...].astype(jnp.int32)
    out = total[:height]
    for k in range(1, 4):
        out = out + total[k * height : (k + 1) * height] * (1 << (8 * k))
    list_ref[0:height] = jnp.where(out == 0, rows << 15, out)


def gather_kernel(
    sizes, q_ref, table_ref, len_ref, all_ref, list_ref, pos_ref, code_ref, total_ref, own_sem,
    send, recv
):
    side, y, z = place()

    def view(q, of, at_y, at_z):
        f, g = (at_y, at_z) if q < 2 else (at_z, at_y)
        return all_ref.at[q, around(f), of, around(g)]

    own = [
        pltpu.make_async_copy(q_ref.at[q], view(q, side, y, z), own_sem.at[q]) for q in range(4)
    ]
    for copy in own:
        copy.start()
    greet(near())
    for copy in own:
        copy.wait()
    slots, rows = table_ref.shape

    def between(level, plane):
        if level == 0:
            plan_start(sizes, table_ref, len_ref, list_ref, pos_ref, code_ref, total_ref)
        if level < 4:
            plan_collect(
                level * slots // 4, (level + 1) * slots // 4, pos_ref, code_ref, total_ref
            )
        else:
            plan_finish(list_ref, total_ref, rows)
            for j in range(RING):
                plane(j)

    torus_gather(view, send, recv, between)


def gather_queries(queries, table, lengths, sizes):
    rows, q_local, head_dim = queries.shape
    dma = pltpu.SemaphoreType.DMA
    vmem = pl.BlockSpec(memory_space=pltpu.VMEM)
    return pl.pallas_call(
        functools.partial(gather_kernel, sizes),
        out_shape=(
            jax.ShapeDtypeStruct((4, RING, 2, RING, rows // 4, q_local, head_dim), queries.dtype),
            jax.ShapeDtypeStruct((LISTED // 128 + 8, 128), jnp.int32),
        ),
        in_specs=[vmem] * 3,
        out_specs=(vmem, vmem),
        scratch_shapes=[
            pltpu.VMEM(table.shape, jnp.int32), pltpu.VMEM(table.shape, jnp.int32),
            pltpu.VMEM((LISTED // 32, 128), jnp.float32), dma((4,)),
        ] + torus_sems(),
        compiler_params=pltpu.CompilerParams(collective_id=0, has_side_effects=True, vmem_limit_bytes=8 << 20),
        cost_estimate=pl.CostEstimate(flops=20_000_000_000, bytes_accessed=8 << 20, transcendentals=0),
    )(queries.reshape(4, rows // 4, q_local, head_dim), table, lengths)


def attend_kernel(
    sizes, listed, q_ref, kbuf, vbuf, acc_turned, stat_turned,
    acc_ref, stat_ref,
):
    kv_local, blocks = sizes
    rows, q_local, head_dim = q_ref.shape
    pages, span, _ = kbuf.shape
    f32, i32 = jnp.float32, jnp.int32
    tall = GROUP * q_local
    wide = GROUP * span
    whole_lane = lax.broadcasted_iota(i32, (128, 128), 1)

    @pl.loop(0, blocks)
    def _(b):
        acc_ref[b] = jnp.zeros(acc_ref.shape[1:], f32)
        stat_ref[b] = jnp.where(whole_lane % 2 == 0, NEG, 0.0)

    lane = lax.broadcasted_iota(i32, (tall, wide), 1)
    line = lax.broadcasted_iota(i32, (tall, wide), 0)
    fits = (lane // span == line // q_local) & (
        lane % kv_local == (line % q_local) // (q_local // kv_local)
    )
    token = jnp.where(fits, (lane % span) // kv_local, 64)
    stat_lane = lax.broadcasted_iota(i32, (q_local, 128), 1)
    scale = head_dim ** (-0.5)

    def half(first):
        codes = [listed[first + i] for i in range(GROUP)]
        used = [code & 31 for code in codes]
        page = [(code >> 5) & (pages - 1) for code in codes]
        row = [code >> 15 for code in codes]
        asked = jnp.concatenate([q_ref[r & (rows - 1)] for r in row], axis=0)
        keys = jnp.concatenate([kbuf[p] for p in page], axis=0)
        values = jnp.concatenate([vbuf[p] for p in page], axis=0)
        limit = jnp.concatenate([jnp.full((q_local, wide), u, i32) for u in used], axis=0)
        return row, asked, keys, values, token < limit

    def soft(scores, valid):
        scores = jnp.where(valid, scores * scale, NEG)
        peak = jnp.max(scores, axis=1, keepdims=True)
        weights = jnp.where(valid, jnp.exp(scores - peak), 0.0)
        return peak, jnp.sum(weights, axis=1, keepdims=True), weights.astype(jnp.bfloat16)

    def quad(firsts):
        halves = [half(first) for first in firsts]
        scores = [
            lax.dot_general(h[1], h[2], (((1,), (1,)), ((), ())), preferred_element_type=f32)
            for h in halves
        ]
        soft_of = [soft(x, h[4]) for x, h in zip(scores, halves)]
        none = jnp.zeros((tall, wide), jnp.bfloat16)
        if len(halves) == 1:
            left, right = soft_of[0][2], halves[0][3]
        else:
            left = jnp.concatenate([
                jnp.concatenate([x[2], none] if k % 2 == 0 else [none, x[2]], axis=1)
                for k, x in enumerate(soft_of)
            ], axis=0)
            right = jnp.concatenate([
                jnp.concatenate([halves[k][3], halves[k + 1][3]], axis=0)
                for k in range(0, len(halves), 2)
            ], axis=1)
        acc = jnp.dot(left, right, preferred_element_type=f32)
        out = []
        for k in range(len(halves)):
            part = acc[k * tall : (k + 1) * tall, (k // 2) * head_dim : (k // 2 + 1) * head_dim]
            for i in range(GROUP):
                at = slice(i * q_local, (i + 1) * q_local)
                out.append((halves[k][0][i], soft_of[k][0][at], soft_of[k][1][at], part[at]))
        return out

    def split(row):
        first = pl.multiple_of((row & 7) * q_local, q_local)
        peak_here = stat_lane == ((row >> 3) & 3) * 2
        mass_here = stat_lane == ((row >> 3) & 3) * 2 + 1
        return row >> 5, row & 31, pl.ds(first, q_local), peak_here, mass_here

    def batch(first):
        parts = []
        for k in range(0, BATCH, 4 * GROUP):
            parts += quad([first + k + u * GROUP for u in range(4)])
        return parts

    def put(row, peak, mass, acc):
        block, at, lines, peak_here, mass_here = split(row)
        acc_ref[block, at] = acc
        pltpu.store(
            stat_ref.at[block, lines], jnp.where(peak_here, peak, mass), mask=peak_here | mass_here
        )

    def merged(row, peak, mass, acc):
        block, at, lines, peak_here, mass_here = split(row)
        old = stat_ref[block, lines]
        old_peak = jnp.max(jnp.where(peak_here, old, NEG), axis=1, keepdims=True)
        old_mass = jnp.sum(jnp.where(mass_here, old, 0.0), axis=1, keepdims=True)
        top = jnp.maximum(old_peak, peak)
        old_f = jnp.exp(old_peak - top)
        new_f = jnp.exp(peak - top)
        return row, top, old_mass * old_f + mass * new_f, acc_ref[block, at] * old_f + acc * new_f

    @pl.loop(0, (listed[LISTED] + BATCH - 1) // BATCH)
    def _(i):
        for part in batch(i * BATCH):
            put(*part)

    for count, first, by in (
        (listed[LISTED + 128], SECOND - BATCH, -BATCH), (listed[LISTED + 256], THIRD, BATCH),
    ):
        @pl.loop(0, (count + BATCH - 1) // BATCH)
        def _(i):
            for part in [merged(*part) for part in batch(first + i * by)]:
                put(*part)

    @pl.loop(0, (listed[LISTED + 384] + GROUP - 1) // GROUP)
    def _(i):
        for part in quad([LATER + i * GROUP]):
            put(*merged(*part))

    eighth = 128 // q_local

    @pl.loop(0, blocks - 1)
    def _(b):
        for g in range(4):
            tile = acc_ref[b, g * eighth : (g + 1) * eighth].reshape(128, head_dim)
            acc_turned[b, g] = tile.T
        stat_turned[b] = stat_ref[b].T[:8]


def attend(listed, queries, keys, values, kv_local):
    rows, q_local, head_dim = queries.shape
    blocks = rows // 32 + 1
    f32 = jnp.float32
    vmem = pl.BlockSpec(memory_space=pltpu.VMEM)
    return pl.pallas_call(
        functools.partial(attend_kernel, (kv_local, blocks)),
        out_shape=(
            jax.ShapeDtypeStruct((blocks - 1, 4, head_dim, 128), f32),
            jax.ShapeDtypeStruct((blocks - 1, 8, 128), f32),
        ),
        in_specs=[pl.BlockSpec(memory_space=pltpu.SMEM), vmem, vmem, vmem],
        out_specs=(vmem, vmem),
        scratch_shapes=[
            pltpu.VMEM((blocks, 32, q_local, head_dim), f32),
            pltpu.VMEM((blocks, 128, 128), f32),
        ],
        compiler_params=pltpu.CompilerParams(vmem_limit_bytes=16 << 20),
    )(listed, queries, keys, values)


def finish_kernel(
    acc_hbm, stat_hbm, w_hbm, att_out, proj_out,
    got_acc, got_stat, out_code, out_stat, in_code, in_stat,
    last_code, last_stat, weight, mixed, everyone, own_part, part_out, part_step_out, part_in, part_step_in,
    cross_send, cross_recv, hop_send, hop_recv, last_send, last_recv, w_sem,
    part_send, part_recv,
    torus_send, torus_recv,
):
    n = lax.axis_size("dp")
    me = lax.axis_index("dp")
    m = lax.axis_size("mp")
    mine = lax.axis_index("mp")
    side, y, z = place()
    rows, q_local, head_dim = att_out.shape
    out_rows = proj_out.shape[0]
    f32 = jnp.float32
    load_w = pltpu.make_async_copy(w_hbm, weight, w_sem)
    load_w.start()

    def axes(q):
        return jnp.where(q < 2, y, z), jnp.where(q < 2, z, y), 1 - 2 * lax.rem(q, 2)

    def first_axis(q, i):
        return {"dp": jnp.where(q < 2, spot(side, y + i, z), spot(side, y, z + i))}

    def second_axis(q, i):
        return {"dp": jnp.where(q < 2, spot(side, y, z + i), spot(side, y + i, z))}

    def block_of(kind, q, of):
        f, _, d = axes(q)
        f = around(f + jnp.where(kind == 0, 2, jnp.where(kind == 1, -d, jnp.where(kind == 2, d, 0))))
        return (q * RING + f) * 2 + of

    def cross_copies(kind, q):
        at = block_of(kind, q, 1 - side)
        peer = {"dp": spot(1 - side, y, z)}
        return (
            remote(acc_hbm.at[at], got_acc.at[kind, q], cross_send.at[0, kind, q],
                   cross_recv.at[0, kind, q], peer),
            remote(stat_hbm.at[at], got_stat.at[kind, q], cross_send.at[1, kind, q],
                   cross_recv.at[1, kind, q], peer),
        )

    def hop_copies(kind, q):
        _, _, d = axes(q)
        peer = first_axis(q, jnp.where(kind == 1, -d, d))
        return (
            remote(out_code.at[kind, q], in_code.at[kind, q], hop_send.at[0, kind, q],
                   hop_recv.at[0, kind, q], peer),
            remote(out_stat.at[kind, q], in_stat.at[kind, q], hop_send.at[1, kind, q],
                   hop_recv.at[1, kind, q], peer),
        )

    def last_copies(o, q):
        _, g, _ = axes(q)
        peer = second_axis(q, o)
        at = around(g + o)
        return (
            remote(out_code.at[3, q, at], last_code.at[o - 1, q],
                   last_send.at[0, o - 1, q], last_recv.at[0, o - 1, q], peer),
            remote(out_stat.at[3, q, at], last_stat.at[o - 1, q],
                   last_send.at[1, o - 1, q], last_recv.at[1, o - 1, q], peer),
        )

    peers = near() + [{"dp": spot(side, y + 2, z)}, {"dp": spot(side, y, z + 2)}]
    peers += [{"mp": lax.rem(mine + i, m)} for i in range(1, m)]
    greet(peers)

    @pl.loop(0, 16)
    def _(i):
        for copy in cross_copies(i // 4, lax.rem(i, 4)):
            copy.start()

    def combine(parts):
        top = parts[0][0]
        for part in parts[1:]:
            top = jnp.maximum(top, part[0])
        mass = 0.0
        gains = []
        for its_top, its_mass, step in parts:
            factor = jnp.exp(its_top - top)
            mass = mass + factor * its_mass
            gains.append(factor if step is None else factor * step)
        return top, mass, gains

    def coded(tile):
        return tile[0:1], tile[1:2], tile[2:3]

    def encode(value):
        step = jnp.max(jnp.abs(value), axis=0, keepdims=True) * (1.0 / 32767.0)
        floor = jnp.maximum(step, 1e-30)
        inverse = 1.0 / floor
        inverse = jnp.where(step > 1e-30, inverse * (2.0 - floor * inverse), 0.0)
        return jnp.round(value * inverse).astype(jnp.int32).astype(jnp.int16), step

    def gathered(kind, q, arrived):
        own = block_of(kind, q, side)
        for copy in cross_copies(kind, q):
            copy.wait_recv()
        for other in arrived:
            for copy in hop_copies(other, q):
                copy.wait_recv()
        for g in range(4):
            plain = [
                (stat[2 * g : 2 * g + 1], stat[2 * g + 1 : 2 * g + 2], None)
                for stat in (stat_hbm[own], got_stat[kind, q])
            ]
            top, mass, gains = combine(plain + [coded(in_stat[k, q, g]) for k in arrived])
            value = acc_hbm[own, g] * gains[0] + got_acc[kind, q, g] * gains[1]
            for gain, k in zip(gains[2:], arrived):
                value = value + in_code[k, q, g].astype(f32) * gain
            out_code[kind, q, g], step = encode(value)
            out_stat[kind, q, g, 0:1] = top
            out_stat[kind, q, g, 1:2] = mass
            out_stat[kind, q, g, 2:3] = step

    @pl.loop(0, 8)
    def _(i):
        kind, q = i // 4, lax.rem(i, 4)
        gathered(kind, q, ())
        for copy in hop_copies(kind, q):
            copy.start()

    @pl.loop(0, 4)
    def _(q):
        gathered(2, q, (0,))
        for copy in hop_copies(2, q):
            copy.start()

    @pl.loop(0, 4)
    def _(q):
        gathered(3, q, (1, 2))
        for o in (2, 1, 3):
            for copy in last_copies(o, q):
                copy.start()

    @pl.loop(0, 4)
    def _(q):
        _, g, _ = axes(q)
        parts = [coded(out_stat[3, q, g])]
        for o in range(1, 4):
            for copy in last_copies(o, q):
                copy.wait_recv()
            parts.append(coded(last_stat[o - 1, q]))
        _, mass, gains = combine(parts)
        value = out_code[3, q, g].astype(f32) * (gains[0] / mass)
        for o in range(1, 4):
            value = value + last_code[o - 1, q].astype(f32) * (gains[o] / mass)
        mixed[pl.ds(q * (rows // 4), rows // 4)] = value.T.reshape(rows // 4, q_local, head_dim)

    att_out[...] = mixed[...].astype(jnp.bfloat16)
    for h in range(q_local):
        at = (h % 4) * head_dim
        everyone[me, h // 4, :, at : at + head_dim] = mixed[:, h, :].astype(jnp.bfloat16)

    band = q_local * head_dim // 4
    homes = n // m

    def part_copies(j, slot):
        target = {"mp": around(z + j)}
        return (
            remote(part_out.at[j], part_in.at[slot], part_send.at[0, j], part_recv.at[0, slot], target),
            remote(part_step_out.at[j], part_step_in.at[slot], part_send.at[1, j],
                   part_recv.at[1, slot], target),
        )

    def project(j):
        owner = around(z + j)
        at = pl.multiple_of(owner * homes, homes)
        value = 0.0
        for q in range(4):
            value += jnp.dot(
                everyone[pl.ds(at, homes), q].reshape(out_rows, band),
                weight[q * band : (q + 1) * band], preferred_element_type=f32,
            )

        @pl.when(owner == mine)
        def _():
            own_part[...] = value

        @pl.when(owner != mine)
        def _():
            part_out[j], step = encode(value)
            part_step_out[j, 0:1] = step
            for copy in part_copies(j, around(mine - owner)):
                copy.start()

    def between(level, plane):
        if level == 1:
            load_w.wait()
        for j in {2: (0,), 3: (1, 3), 4: (2,)}.get(level, ()):
            plane(j)
            project(j)

    torus_gather(
        lambda q, of, at_y, at_z: everyone.at[spot(of, at_y, at_z), q], torus_send, torus_recv,
        between,
    )
    total = own_part[...]
    for slot in range(1, m):
        for copy in part_copies(0, slot):
            copy.wait_recv()
        total = total + part_in[slot].astype(f32) * part_step_in[slot, 0:1]
    proj_out[...] = total.astype(jnp.bfloat16)
    for j in range(m):
        @pl.when(around(z + j) != mine)
        def _():
            for copy in part_copies(j, 1):
                copy.wait_send()

    @pl.loop(0, 16)
    def _(i):
        for copy in cross_copies(i // 4, lax.rem(i, 4)):
            copy.wait_send()

    @pl.loop(0, 12)
    def _(i):
        kind, q = i // 4, lax.rem(i, 4)
        for copy in hop_copies(kind, q) + last_copies(kind + 1, q):
            copy.wait_send()


def finish(acc, stat, out_weight, q_local):
    _, _, head_dim, _ = acc.shape
    rows = 4 * 128 // q_local
    n = lax.axis_size("dp")
    m = lax.axis_size("mp")
    depth, columns = out_weight.shape
    out_rows = n * rows // m
    dma = pltpu.SemaphoreType.DMA
    f32, i16 = jnp.float32, jnp.int16
    return pl.pallas_call(
        finish_kernel,
        out_shape=(
            jax.ShapeDtypeStruct((rows, q_local, head_dim), jnp.bfloat16),
            jax.ShapeDtypeStruct((out_rows, columns), jnp.bfloat16),
        ),
        in_specs=[pl.BlockSpec(memory_space=pltpu.VMEM)] * 2 + [pl.BlockSpec(memory_space=pl.ANY)],
        out_specs=(pl.BlockSpec(memory_space=pltpu.VMEM),) * 2,
        scratch_shapes=[
            pltpu.VMEM((4, 4, 4, head_dim, 128), f32),
            pltpu.VMEM((4, 4, 8, 128), f32),
            pltpu.VMEM((4, 4, 4, head_dim, 128), i16),
            pltpu.VMEM((4, 4, 4, 4, 128), f32),
            pltpu.VMEM((3, 4, 4, head_dim, 128), i16),
            pltpu.VMEM((3, 4, 4, 4, 128), f32),
            pltpu.VMEM((3, 4, head_dim, 128), i16),
            pltpu.VMEM((3, 4, 4, 128), f32),
            pltpu.VMEM((depth, columns), out_weight.dtype),
            pltpu.VMEM((rows, q_local, head_dim), f32),
            pltpu.VMEM((n, 4, rows, q_local * head_dim // 4), jnp.bfloat16),
            pltpu.VMEM((out_rows, columns), f32),
            pltpu.VMEM((m, out_rows, columns), i16),
            pltpu.VMEM((m, 8, columns), f32),
            pltpu.VMEM((m, out_rows, columns), i16),
            pltpu.VMEM((m, 8, columns), f32),
            dma((2, 4, 4)), dma((2, 4, 4)),
            dma((2, 3, 4)), dma((2, 3, 4)), dma((2, 3, 4)), dma((2, 3, 4)), dma,
            dma((2, m)), dma((2, m)),
        ] + torus_sems(),
        compiler_params=pltpu.CompilerParams(collective_id=1, has_side_effects=True, vmem_limit_bytes=24 << 20),
    )(acc, stat, out_weight)


def shards(queries, lookup_sheets, content_sheets, page_table, context_len, out_weight):
    req_rows = page_table.shape[0]
    pool_local, page_len, kv_local, head_dim = lookup_sheets.shape
    span = page_len * kv_local
    all_queries, listed = gather_queries(
        queries, page_table.T, context_len.reshape(1, req_rows), (pool_local, page_len)
    )
    acc, stat = attend(
        listed.reshape(-1), all_queries.reshape(req_rows, *queries.shape[1:]),
        lookup_sheets.reshape(pool_local, span, head_dim),
        content_sheets.reshape(pool_local, span, head_dim), kv_local,
    )
    return finish(acc, stat, out_weight, queries.shape[1])


def solution(mesh):
    placed = (
        P("dp", "mp", None),
        P("dp", None, "mp", None),
        P("dp", None, "mp", None),
        P(),
        P(),
        P("mp", "dp"),
    )
    return jax.shard_map(
        shards,
        mesh=mesh,
        in_specs=placed,
        out_specs=(P("dp", "mp", None), P("mp", "dp")),
        check_vma=False,
    )
```
